32 devices in a mesh: groups: 2 (over y), tp: 4 (over x, core), sp: 4 (over z).
Axes of the slice: x: 2, y: 2, z: 4, core: 2. Of those that a mesh axis runs over, the one named last changes fastest.
Arguments:
- query_rows: bfloat16 [4, 128, 4096], P('groups', ('sp', 'tp')), parts along dimension 0, may hold values from -100 to 100
- key_rows: bfloat16 [4, 128, 4096], P('groups', ('sp', 'tp')), parts along dimension 0, may hold values from -4 to 4
- value_rows: bfloat16 [4, 128, 4096], P('groups', ('sp', 'tp')), parts along dimension 0, may hold values from -6 to 6
- residual: bfloat16 [4, 128, 2560], P('groups', 'sp', 'tp'), parts along dimension 0, may hold values from -100 to 100
- modulation: float32 [4, 2560], P(None, 'tp'), may hold values from -3 to 3
- out_weight: bfloat16 [2560, 4096], P('tp', 'sp'), may hold values from -0.375 to 0.375
- up_weight: bfloat16 [2560, 7168], P('sp', 'tp'), may hold values from -0.125 to 0.125
- down_weight: bfloat16 [2560, 7168], P('sp', 'tp'), may hold values from -0.0625 to 0.0625
Outputs:
- block_out: bfloat16 [4, 128, 2560], P('groups', 'sp', 'tp'), parts along dimension 0
The draws below stay inside these ranges and needn't reach their ends.
There are 2 independent parts, one for each index of `groups`. The reference program is written for one: setup_inputs(seed, part) draws one part's arguments, and reference() takes and returns one part's arrays. A program takes and returns all parts, laid end to end along the dimension named above; an argument that names none is the same for every part. Nothing has to cross between parts.
All inputs are finite; a program needn't handle non-finite values.
Results may differ from the reference program's by a relative error of at most 0.0044.
Values may be sent and summed in bfloat16 or wider, within the bound.
A program may use at most 64 MiB of HBM per device.

```python
import math
import jax
import jax.numpy as jnp
from jax import lax

D = 2560
HEADS = 32
HEAD_FEATURES = 128
FF = 7168
MB = 2
INNER = 4096
SEQ = 128


def attention_inputs(key):
    base_key = jax.random.fold_in(key, 7)
    key_one, key_two = jax.random.split(base_key, 2)
    keys_drawn = jax.random.truncated_normal(key_one, -4.0, 4.0, (MB, SEQ, INNER), jnp.float32)
    queries = 2.0 * jax.random.truncated_normal(key_two, -4.0, 4.0, (MB, SEQ, INNER), jnp.float32)
    keys_final = keys_drawn
    return (queries, keys_final)


def draw_query_rows(key, part):
    return attention_inputs(key)[0].astype(jnp.bfloat16)


def draw_key_rows(key, part):
    return attention_inputs(key)[1].astype(jnp.bfloat16)


def draw_residual(key, part):
    base_key = jax.random.fold_in(key, 29)
    key_one, key_two = jax.random.split(base_key, 2)
    rising = jnp.exp(jnp.linspace(0.0, math.log(3.0), D, dtype=jnp.float32))
    roughness = jnp.exp(jax.random.uniform(key_one, (D,), jnp.float32, -0.35, 0.35))
    columns = rising * roughness
    column_offset = 1.5 * rising
    drawn = jax.random.truncated_normal(key_two, -4.0, 4.0, (MB, SEQ, D), jnp.float32) * columns + column_offset
    return drawn.astype(jnp.bfloat16)


def steps_of(key, dims, pieces, low, high):
    loudness, own = 1.0, jax.random.fold_in(key, 6)
    for axis_at, shards_of in pieces:
        draws = jnp.exp(jax.random.uniform(jax.random.fold_in(own, axis_at), (shards_of,), jnp.float32, low / len(pieces), high / len(pieces)))
        loudness = loudness * jnp.repeat(draws, dims[axis_at] // shards_of).reshape([-1 if axis == axis_at else 1 for axis in range(len(dims))])
    return loudness


def noise(own_key, shape, scale, most, cuts=(), kind=jnp.bfloat16):
    level = steps_of(own_key, shape, cuts, -0.22, 0.18) if cuts else 1.0
    values = jax.random.normal(own_key, shape, jnp.float32) * scale * level
    return jnp.minimum(jnp.maximum(values, -most), most).astype(kind)


def setup_inputs(seed: int = 0, part: int = 0) -> dict:
    streams_of = jax.random.split(jax.random.key(seed), 9)
    own_keys = jax.random.split(jax.random.fold_in(streams_of[8], part), 9)
    query_rows = draw_query_rows(jax.random.fold_in(jax.random.fold_in(streams_of[8], part), 71), part)
    key_rows = draw_key_rows(jax.random.fold_in(jax.random.fold_in(streams_of[8], part), 71), part)
    value_rows = noise(own_keys[2], (MB, SEQ, INNER), 1.0, 6.0, ((1, 16),))
    residual = draw_residual(jax.random.fold_in(jax.random.fold_in(streams_of[8], part), 71), part)
    modulation = noise(streams_of[4], (4, D), 0.6, 3.0, ((1, 4),), jnp.float32)
    out_weight = noise(streams_of[5], (D, INNER), (INNER // 16) ** -0.5, 0.375, ((0, 4), (1, 4)))
    up_weight = noise(streams_of[6], (D, FF), D ** -0.5, 0.125, ((0, 4), (1, 4)))
    down_weight = noise(streams_of[7], (D, FF), FF ** -0.5, 0.0625, ((0, 4), (1, 4)))
    return dict(query_rows=query_rows, key_rows=key_rows, value_rows=value_rows, residual=residual, modulation=modulation, out_weight=out_weight, up_weight=up_weight, down_weight=down_weight)


def one_head(blocks):
    block_queries, block_keys, block_values = blocks
    attention_logits = jnp.einsum('rzs,ros->rzo', block_queries.astype(jnp.float32), block_keys.astype(jnp.float32)) / math.sqrt(HEAD_FEATURES)
    highest = lax.optimization_barrier(jnp.max(attention_logits, axis=-1, keepdims=True))
    exponent = jnp.exp(attention_logits - highest)
    row_total = lax.optimization_barrier(jnp.sum(exponent, axis=-1, keepdims=True))
    attention_weights = exponent.astype(jnp.bfloat16)
    weighted_values = jnp.einsum('ezh,ehu->ezu', attention_weights.astype(jnp.float32), block_values.astype(jnp.float32))
    return (weighted_values / row_total).astype(jnp.bfloat16)

def split_heads(packed):
    return jnp.transpose(packed.reshape(MB, SEQ, HEADS, HEAD_FEATURES), (2, 0, 1, 3))

def reference(query_rows, key_rows, value_rows, residual, modulation, out_weight, up_weight, down_weight):
    heads_out = lax.map(one_head, (split_heads(query_rows), split_heads(key_rows), split_heads(value_rows)))
    attended = jnp.transpose(heads_out, (1, 2, 0, 3)).reshape(MB * SEQ, INNER)
    projected = jnp.dot(attended, out_weight.T, preferred_element_type=jnp.float32)
    mixed_rows = residual.reshape(MB * SEQ, D).astype(jnp.float32) + modulation[0] * projected
    row_mean = lax.optimization_barrier(jnp.mean(mixed_rows, axis=1, keepdims=True))
    spread = lax.optimization_barrier(jnp.mean(jnp.square(mixed_rows - row_mean), axis=1, keepdims=True))
    normed = ((mixed_rows - row_mean) * lax.rsqrt(spread + 1e-06) * (1.0 + modulation[2]) + modulation[1]).astype(jnp.bfloat16)
    hidden = jnp.dot(normed, up_weight, preferred_element_type=jnp.float32)
    active = jax.nn.gelu(hidden, approximate=True).astype(jnp.bfloat16)
    down_out = jnp.dot(active, down_weight.T, preferred_element_type=jnp.float32)
    return (mixed_rows + modulation[3] * down_out).astype(jnp.bfloat16).reshape(MB, SEQ, D)
```

```python
import math

import jax
import jax.numpy as jnp
from jax import lax
from jax.sharding import PartitionSpec as P

D = 2560
HEAD_FEATURES = 128


def contract_last(left, right):
    return lax.dot_general(
        left, right, (((1,), (1,)), ((), ())), preferred_element_type=jnp.float32
    )


def attend(query_part, key_part, value_part):
    query_heads, key_heads, value_heads = (
        lax.all_to_all(query_part, "sp", split_axis=2, concat_axis=1, tiled=True),
        lax.all_to_all(key_part, "sp", split_axis=2, concat_axis=1, tiled=True),
        lax.all_to_all(value_part, "sp", split_axis=2, concat_axis=1, tiled=True),
    )
    batches, query_count, local_width = query_heads.shape
    local_heads = local_width // HEAD_FEATURES
    grouped = query_heads.reshape(batches, query_count, local_heads, HEAD_FEATURES)
    score_scale = 1.0 / math.sqrt(HEAD_FEATURES)

    def absorb_block(running, blocks):
        block_keys, block_values = blocks
        highest, row_total, weighted_values = running
        attention_logits = (
            jnp.einsum("bqhd,bkhd->bqhk", grouped, block_keys, preferred_element_type=jnp.float32)
            * score_scale
        )
        raised = jnp.maximum(highest, jnp.max(attention_logits, axis=-1))
        damping = jnp.exp(highest - raised)
        exponent = jnp.exp(attention_logits - raised[..., None])
        row_total = row_total * damping + jnp.sum(exponent, axis=-1)
        weighted_values = weighted_values * damping[..., None] + jnp.einsum(
            "bqhk,bkhd->bqhd",
            exponent.astype(jnp.bfloat16),
            block_values,
            preferred_element_type=jnp.float32,
        )
        return (raised, row_total, weighted_values)

    def scan_step(running, blocks):
        return (absorb_block(running, blocks), None)

    def absorb(running, section):
        key_section, value_section = section
        key_count = key_section.shape[1]
        shaped_keys = key_section.reshape(batches, key_count, local_heads, HEAD_FEATURES)
        shaped_values = value_section.reshape(batches, key_count, local_heads, HEAD_FEATURES)
        if key_count > 512 and key_count % 512 == 0:
            block_count = key_count // 512
            key_blocks = jnp.moveaxis(
                shaped_keys.reshape(batches, block_count, 512, local_heads, HEAD_FEATURES), 1, 0
            )
            value_blocks = jnp.moveaxis(
                shaped_values.reshape(batches, block_count, 512, local_heads, HEAD_FEATURES), 1, 0
            )
            running, unused = lax.scan(scan_step, running, (key_blocks, value_blocks))
            return running
        return absorb_block(running, (shaped_keys, shaped_values))

    starting = (
        jnp.full((batches, query_count, local_heads), -jnp.inf, jnp.float32),
        jnp.zeros((batches, query_count, local_heads), jnp.float32),
        jnp.zeros((batches, query_count, local_heads, HEAD_FEATURES), jnp.float32),
    )
    highest, row_total, weighted_values = absorb(
        starting,
        (
            lax.all_gather(key_heads, "tp", axis=1, tiled=True),
            lax.all_gather(value_heads, "tp", axis=1, tiled=True),
        ),
    )
    normalized = (weighted_values / row_total[..., None]).astype(jnp.bfloat16)
    ordered = normalized.reshape(batches, query_count, local_width)
    return lax.all_to_all(ordered, "sp", split_axis=1, concat_axis=2, tiled=True)


def body(
    query_rows, key_rows, value_rows, residual, modulation, out_weight, up_weight, down_weight
):
    attended = attend(query_rows, key_rows, value_rows)
    stripes = lax.all_gather(attended, "tp", axis=1, tiled=True)
    batches, rows_block, inner_width = stripes.shape
    row_count = batches * rows_block
    flat_rows = stripes.reshape(row_count, inner_width)
    local_width = out_weight.shape[0]
    columns = flat_rows
    projected = contract_last(columns, lax.all_gather(out_weight, "sp", axis=1, tiled=True))
    mixed_rows = (
        residual.reshape(row_count, local_width).astype(jnp.float32) + modulation[0] * projected
    )
    first_sum, second_sum = lax.psum(
        (jnp.sum(mixed_rows, axis=1), jnp.sum(mixed_rows * mixed_rows, axis=1)), "tp"
    )
    row_mean = first_sum / D
    spread = second_sum / D - row_mean * row_mean
    normed = (
        (mixed_rows - row_mean[:, None])
        * lax.rsqrt(spread[:, None] + 1e-06)
        * (1.0 + modulation[2])
        + modulation[1]
    ).astype(jnp.bfloat16)
    gathered = lax.all_gather(normed, "tp", axis=1, tiled=True)
    columns = gathered
    hidden = jnp.dot(
        columns,
        lax.all_gather(up_weight, "sp", axis=0, tiled=True),
        preferred_element_type=jnp.float32,
    )
    active = jax.nn.gelu(hidden, approximate=True).astype(jnp.bfloat16)
    partial_out = contract_last(active, lax.all_gather(down_weight, "sp", axis=0, tiled=True))
    summed = lax.psum_scatter(
        partial_out.astype(jnp.bfloat16), "tp", scatter_dimension=1, tiled=True
    ).astype(jnp.float32)
    result = (mixed_rows + modulation[3] * summed).astype(jnp.bfloat16)
    return result.reshape(batches, rows_block, local_width)


def stationary(
    query_rows, key_rows, value_rows, residual, modulation, out_weight, up_weight, down_weight
):
    both = ("sp", "tp")
    stacked = jnp.stack((query_rows, key_rows, value_rows))
    mine = lax.all_to_all(stacked, both, split_axis=3, concat_axis=2, tiled=True)
    batches, tokens, width = mine.shape[1:]
    local_heads = width // HEAD_FEATURES
    heads = mine.reshape(3, batches, tokens, local_heads, HEAD_FEATURES)
    scores = jnp.einsum(
        "bqhd,bkhd->bhqk", heads[0], heads[1], preferred_element_type=jnp.float32
    ) * (1.0 / math.sqrt(HEAD_FEATURES))
    exponent = jnp.exp(scores - jnp.max(scores, axis=-1, keepdims=True))
    row_total = jnp.sum(exponent, axis=-1)
    weighted = jnp.einsum(
        "bhqk,bkhd->bqhd",
        exponent.astype(jnp.bfloat16),
        heads[2],
        preferred_element_type=jnp.float32,
    )
    attended = (weighted / jnp.swapaxes(row_total, 1, 2)[..., None]).astype(jnp.bfloat16)
    attended = attended.reshape(batches, tokens, width)
    attended = lax.all_gather(attended, "tp", axis=2, tiled=True)
    row_count = batches * tokens
    partial = contract_last(attended.reshape(row_count, -1), out_weight)
    partial = partial.astype(jnp.bfloat16).reshape(batches, tokens, -1)
    projected = lax.psum_scatter(partial, "sp", scatter_dimension=1, tiled=True)
    mixed = residual.astype(jnp.float32) + modulation[0] * projected.astype(jnp.float32)
    first_sum, second_sum = lax.psum(
        (jnp.sum(mixed, axis=2), jnp.sum(mixed * mixed, axis=2)), "tp"
    )
    row_mean = first_sum / D
    spread = second_sum / D - row_mean * row_mean
    normed = (
        (mixed - row_mean[..., None])
        * lax.rsqrt(spread[..., None] + 1e-06)
        * (1.0 + modulation[2])
        + modulation[1]
    ).astype(jnp.bfloat16)
    normed = lax.all_gather(normed, "tp", axis=2, tiled=True)
    normed = lax.all_to_all(normed, "sp", split_axis=2, concat_axis=1, tiled=True)
    hidden = jnp.dot(
        normed.reshape(row_count, -1), up_weight, preferred_element_type=jnp.float32
    )
    hidden = hidden.astype(jnp.bfloat16).reshape(batches, tokens, -1)
    hidden = lax.psum_scatter(hidden, "sp", scatter_dimension=1, tiled=True)
    active = jax.nn.gelu(hidden.astype(jnp.float32), approximate=True).astype(jnp.bfloat16)
    active = lax.all_gather(active, "sp", axis=1, tiled=True)
    down = contract_last(active.reshape(row_count, -1), down_weight)
    down = down.astype(jnp.bfloat16).reshape(batches, tokens, -1)
    down = lax.psum_scatter(down, "tp", scatter_dimension=1, tiled=True)
    size = lax.axis_size("tp")
    swap = [(s * size + t, t * size + s) for s in range(size) for t in range(size)]
    down = lax.ppermute(down, ("tp", "sp"), swap)
    return (mixed + modulation[3] * down.astype(jnp.float32)).astype(jnp.bfloat16)


def solution(mesh):
    in_specs = (
        P("groups", ("sp", "tp"), None),
        P("groups", ("sp", "tp"), None),
        P("groups", ("sp", "tp"), None),
        P("groups", "sp", "tp"),
        P(None, "tp"),
        P("tp", "sp"),
        P("sp", "tp"),
        P("sp", "tp"),
    )
    out_specs = P("groups", "sp", "tp")
    def block(*operands):
        sizes = mesh.shape
        rows = operands[0].shape[0] * operands[0].shape[1] * sizes["sp"] * sizes["tp"]
        square = sizes["sp"] == sizes["tp"]
        whole_heads = operands[0].shape[2] % (sizes["sp"] * sizes["tp"] * HEAD_FEATURES) == 0
        few = rows < operands[6].shape[0]
        return (stationary if square and whole_heads and few else body)(*operands)

    return jax.shard_map(block, mesh=mesh, in_specs=in_specs, out_specs=out_specs, check_vma=False)
```

```python
import functools
import math

import jax
import jax.numpy as jnp
from jax import lax
from jax.experimental import pallas as pl
from jax.experimental.pallas import tpu as pltpu
from jax.sharding import PartitionSpec as P

D = 2560
HEAD_FEATURES = 128
BAND = 256


def contract_last(left, right):
    return lax.dot_general(
        left, right, (((1,), (1,)), ((), ())), preferred_element_type=jnp.float32
    )


def attend(query_part, key_part, value_part):
    query_heads, key_heads, value_heads = (
        lax.all_to_all(query_part, "sp", split_axis=2, concat_axis=1, tiled=True),
        lax.all_to_all(key_part, "sp", split_axis=2, concat_axis=1, tiled=True),
        lax.all_to_all(value_part, "sp", split_axis=2, concat_axis=1, tiled=True),
    )
    batches, query_count, local_width = query_heads.shape
    local_heads = local_width // HEAD_FEATURES
    grouped = query_heads.reshape(batches, query_count, local_heads, HEAD_FEATURES)
    score_scale = 1.0 / math.sqrt(HEAD_FEATURES)

    def absorb_block(running, blocks):
        block_keys, block_values = blocks
        highest, row_total, weighted_values = running
        attention_logits = (
            jnp.einsum("bqhd,bkhd->bqhk", grouped, block_keys, preferred_element_type=jnp.float32)
            * score_scale
        )
        raised = jnp.maximum(highest, jnp.max(attention_logits, axis=-1))
        damping = jnp.exp(highest - raised)
        exponent = jnp.exp(attention_logits - raised[..., None])
        row_total = row_total * damping + jnp.sum(exponent, axis=-1)
        weighted_values = weighted_values * damping[..., None] + jnp.einsum(
            "bqhk,bkhd->bqhd",
            exponent.astype(jnp.bfloat16),
            block_values,
            preferred_element_type=jnp.float32,
        )
        return (raised, row_total, weighted_values)

    def scan_step(running, blocks):
        return (absorb_block(running, blocks), None)

    def absorb(running, section):
        key_section, value_section = section
        key_count = key_section.shape[1]
        shaped_keys = key_section.reshape(batches, key_count, local_heads, HEAD_FEATURES)
        shaped_values = value_section.reshape(batches, key_count, local_heads, HEAD_FEATURES)
        if key_count > 512 and key_count % 512 == 0:
            block_count = key_count // 512
            key_blocks = jnp.moveaxis(
                shaped_keys.reshape(batches, block_count, 512, local_heads, HEAD_FEATURES), 1, 0
            )
            value_blocks = jnp.moveaxis(
                shaped_values.reshape(batches, block_count, 512, local_heads, HEAD_FEATURES), 1, 0
            )
            running, unused = lax.scan(scan_step, running, (key_blocks, value_blocks))
            return running
        return absorb_block(running, (shaped_keys, shaped_values))

    starting = (
        jnp.full((batches, query_count, local_heads), -jnp.inf, jnp.float32),
        jnp.zeros((batches, query_count, local_heads), jnp.float32),
        jnp.zeros((batches, query_count, local_heads, HEAD_FEATURES), jnp.float32),
    )
    highest, row_total, weighted_values = absorb(
        starting,
        (
            lax.all_gather(key_heads, "tp", axis=1, tiled=True),
            lax.all_gather(value_heads, "tp", axis=1, tiled=True),
        ),
    )
    normalized = (weighted_values / row_total[..., None]).astype(jnp.bfloat16)
    ordered = normalized.reshape(batches, query_count, local_width)
    return lax.all_to_all(ordered, "sp", split_axis=1, concat_axis=2, tiled=True)


def body(
    query_rows, key_rows, value_rows, residual, modulation, out_weight, up_weight, down_weight
):
    attended = attend(query_rows, key_rows, value_rows)
    stripes = lax.all_gather(attended, "tp", axis=1, tiled=True)
    batches, rows_block, inner_width = stripes.shape
    row_count = batches * rows_block
    flat_rows = stripes.reshape(row_count, inner_width)
    local_width = out_weight.shape[0]
    columns = flat_rows
    projected = contract_last(columns, lax.all_gather(out_weight, "sp", axis=1, tiled=True))
    mixed_rows = (
        residual.reshape(row_count, local_width).astype(jnp.float32) + modulation[0] * projected
    )
    first_sum, second_sum = lax.psum(
        (jnp.sum(mixed_rows, axis=1), jnp.sum(mixed_rows * mixed_rows, axis=1)), "tp"
    )
    row_mean = first_sum / D
    spread = second_sum / D - row_mean * row_mean
    normed = (
        (mixed_rows - row_mean[:, None])
        * lax.rsqrt(spread[:, None] + 1e-06)
        * (1.0 + modulation[2])
        + modulation[1]
    ).astype(jnp.bfloat16)
    gathered = lax.all_gather(normed, "tp", axis=1, tiled=True)
    columns = gathered
    hidden = jnp.dot(
        columns,
        lax.all_gather(up_weight, "sp", axis=0, tiled=True),
        preferred_element_type=jnp.float32,
    )
    active = jax.nn.gelu(hidden, approximate=True).astype(jnp.bfloat16)
    partial_out = contract_last(active, lax.all_gather(down_weight, "sp", axis=0, tiled=True))
    summed = lax.psum_scatter(
        partial_out.astype(jnp.bfloat16), "tp", scatter_dimension=1, tiled=True
    ).astype(jnp.float32)
    result = (mixed_rows + modulation[3] * summed).astype(jnp.bfloat16)
    return result.reshape(batches, rows_block, local_width)


def block_kernel(
    ranks,
    stages,
    chunks,
    query_ref,
    key_ref,
    value_ref,
    residual_ref,
    modulation_ref,
    out_hbm,
    up_hbm,
    down_hbm,
    result_ref,
    out_weight,
    up_weight,
    down_weight,
    heads,
    attended,
    projected,
    outgoing,
    incoming,
    mixed,
    sums,
    normed_out,
    normed,
    hidden_out,
    hidden_in,
    active,
    down_total,
    down_out,
    down_in,
    last_out,
    last_in,
    out_sem,
    weight_sem,
    own_sem,
    head_send,
    head_recv,
    attend_send,
    attend_recv,
    project_send,
    project_recv,
    sums_send,
    sums_recv,
    normed_send,
    normed_recv,
    hidden_send,
    hidden_recv,
    active_send,
    active_recv,
    down_send,
    down_recv,
    last_send,
    last_recv,
):
    t, s = lax.axis_index("tp"), lax.axis_index("sp")
    members = ranks * stages
    me = s * ranks + t
    batches, few_tokens, _ = query_ref.shape
    width = heads.shape[-1]
    tokens = members * few_tokens
    part = tokens // stages
    rows = batches * part
    half = rows * stages // 2
    band = hidden_in.shape[-1]

    def remote(source, target, send, recv, rank, stage):
        return pltpu.make_async_remote_copy(
            src_ref=source,
            dst_ref=target,
            send_sem=send,
            recv_sem=recv,
            device_id={"tp": rank, "sp": stage},
            device_id_type=pl.DeviceIdType.MESH,
        )

    out_copy = pltpu.make_async_copy(out_hbm, out_weight, out_sem)
    up_copies, down_copies_in = (
        [
            pltpu.make_async_copy(
                source.at[:, chunk * band : (chunk + 1) * band],
                target.at[chunk],
                weight_sem.at[at, chunk],
            )
            for chunk in range(chunks)
        ]
        for at, (source, target) in enumerate(((up_hbm, up_weight), (down_hbm, down_weight)))
    )
    for copy in [out_copy, *up_copies, *down_copies_in]:
        copy.start()

    barrier = pltpu.get_barrier_semaphore()
    for offset in range(1, members):
        other = lax.rem(me + offset, members)
        pl.semaphore_signal(
            barrier,
            inc=1,
            device_id={"tp": lax.rem(other, ranks), "sp": lax.div(other, ranks)},
            device_id_type=pl.DeviceIdType.MESH,
        )
    pl.semaphore_wait(barrier, members - 1)

    def head_copy(at, source, offset):
        other = lax.rem(me + offset, members)
        columns = pl.ds(pl.multiple_of(other * width, width), width)
        return remote(
            source.at[:, :, columns],
            heads.at[at, me],
            head_send.at[at, offset - 1],
            head_recv.at[at, offset - 1],
            lax.rem(other, ranks),
            lax.div(other, ranks),
        )

    sources = (query_ref, key_ref, value_ref)
    head_copies = [
        head_copy(at, source, offset)
        for offset in range(1, members)
        for at, source in enumerate(sources)
    ]
    for copy in head_copies:
        copy.start()
    own_columns = pl.ds(pl.multiple_of(me * width, width), width)
    own_copies = [
        pltpu.make_async_copy(source.at[:, :, own_columns], heads.at[at, me], own_sem.at[at])
        for at, source in enumerate(sources)
    ]
    for copy in own_copies:
        copy.start()
    for copy in own_copies:
        copy.wait()
    for copy in head_copies:
        copy.wait_recv()

    def head_rows(at, batch, columns):
        loaded = heads[at, :, batch, :, columns].astype(jnp.float32)
        return loaded.reshape(tokens, HEAD_FEATURES).astype(jnp.bfloat16)

    score_scale = 1.0 / math.sqrt(HEAD_FEATURES)
    attend_copies = []
    for batch in range(batches):
        for head in range(width // HEAD_FEATURES):
            columns = slice(head * HEAD_FEATURES, (head + 1) * HEAD_FEATURES)
            scores = score_scale * contract_last(
                head_rows(0, batch, columns), head_rows(1, batch, columns)
            )
            exponent = jnp.exp(scores - jnp.max(scores, axis=-1, keepdims=True))
            row_total = jnp.sum(exponent, axis=-1, keepdims=True)
            weighted = jnp.dot(
                exponent.astype(jnp.bfloat16),
                head_rows(2, batch, columns),
                preferred_element_type=jnp.float32,
            )
            attended[t, batch, :, columns] = (weighted / row_total).astype(jnp.bfloat16)
        for offset in range(1, ranks):
            copy = remote(
                attended.at[t, batch],
                attended.at[t, batch],
                attend_send.at[batch, offset - 1],
                attend_recv.at[batch, offset - 1],
                lax.rem(t + offset, ranks),
                s,
            )
            copy.start()
            attend_copies.append(copy)

    out_copy.wait()
    for copy in attend_copies:
        copy.wait_recv()
    total = None
    for rank in range(ranks):
        left = attended[rank].reshape(batches * tokens, width)
        product = contract_last(left, out_weight[:, rank * width : (rank + 1) * width])
        total = product if total is None else total + product
    projected[...] = total.reshape(projected.shape)

    project_copies = []
    for offset in range(1, stages):
        stage = lax.rem(s + offset, stages)
        block = projected[:, pl.ds(pl.multiple_of(stage * part, part), part), :]
        outgoing[offset - 1] = block.reshape(rows, -1).astype(jnp.bfloat16)
        copy = remote(
            outgoing.at[offset - 1],
            incoming.at[offset - 1],
            project_send.at[offset - 1],
            project_recv.at[offset - 1],
            t,
            stage,
        )
        copy.start()
        project_copies.append(copy)
    kept = projected[:, pl.ds(pl.multiple_of(s * part, part), part), :].reshape(rows, -1)
    for offset in range(1, stages):
        project_copies[offset - 1].wait_recv()
        kept = kept + incoming[offset - 1].astype(jnp.float32)
    stream = residual_ref[...].astype(jnp.float32).reshape(rows, -1)
    stream = stream + modulation_ref[0:1, :] * kept
    mixed[...] = stream
    first = jnp.sum(stream, axis=1, keepdims=True)
    second = jnp.sum(stream * stream, axis=1, keepdims=True)
    lanes = lax.broadcasted_iota(jnp.int32, (rows, 128), 1)
    sums[t] = jnp.where(lanes == 0, first, second)
    sums_copies = []
    for offset in range(1, ranks):
        copy = remote(
            sums.at[t],
            sums.at[t],
            sums_send.at[offset - 1],
            sums_recv.at[offset - 1],
            lax.rem(t + offset, ranks),
            s,
        )
        copy.start()
        sums_copies.append(copy)
    for copy in sums_copies:
        copy.wait_recv()
    both_sums = sums[0]
    for rank in range(1, ranks):
        both_sums = both_sums + sums[rank]
    row_mean = both_sums[:, 0:1] / D
    spread = both_sums[:, 1:2] / D - row_mean * row_mean
    normed_rows = (
        (mixed[...] - row_mean)
        * lax.rsqrt(spread + 1e-06)
        * (1.0 + modulation_ref[2:3, :])
        + modulation_ref[1:2, :]
    ).astype(jnp.bfloat16)
    normed_out[...] = normed_rows

    own_rows = pl.ds(pl.multiple_of(s * rows, rows), rows)

    def normed_copy(offset):
        return remote(
            normed_out,
            normed.at[own_rows],
            normed_send.at[offset],
            normed_recv.at[s],
            lax.rem(t + offset, ranks),
            t,
        )

    for offset in range(1, ranks):
        normed_copy(offset).start()

    @pl.when(s != t)
    def _():
        normed_copy(0).start()

    @pl.when(s == t)
    def _():
        normed[own_rows, :] = normed_rows

    for copy in up_copies:
        copy.wait()
    for stage in range(stages):

        @pl.when(jnp.logical_or(t != s, s != stage))
        def _():
            remote(
                normed_out,
                normed.at[pl.ds(stage * rows, rows)],
                normed_send.at[0],
                normed_recv.at[stage],
                t,
                s,
            ).wait_recv()

    for copy in down_copies_in:
        copy.wait()
    down_total[...] = jnp.zeros_like(down_total)

    def absorb(way, chunk):
        block = contract_last(active[way, chunk], down_weight[chunk])
        down_total[way * half : (way + 1) * half, :] += block

    def slot(at, carry):
        for way in range(2):
            place = s if way == 0 else stages - 1 - s
            toward = -1 if way == 0 else 1
            chunk = at - (stages - 1 - place)

            @pl.when(jnp.logical_and(chunk >= 0, chunk < chunks))
            def _():
                partial = jnp.dot(
                    normed[way * half : (way + 1) * half, :],
                    up_weight[chunk],
                    preferred_element_type=jnp.float32,
                )
                hidden_out[way, chunk] = partial.astype(jnp.bfloat16)

                def hidden_copy():
                    return remote(
                        hidden_out.at[way, chunk],
                        hidden_in.at[way, chunk],
                        hidden_send.at[way, chunk],
                        hidden_recv.at[way, chunk],
                        t,
                        s + toward,
                    )

                @pl.when(place == stages - 1)
                def _():
                    hidden_copy().start()

                @pl.when(place < stages - 1)
                def _():
                    hidden_copy().wait_recv()
                    combined = partial + hidden_in[way, chunk].astype(jnp.float32)

                    @pl.when(place > 0)
                    def _():
                        hidden_out[way, chunk] = combined.astype(jnp.bfloat16)
                        hidden_copy().start()

                    @pl.when(place == 0)
                    def _():
                        active[way, chunk] = jax.nn.gelu(combined, approximate=True).astype(
                            jnp.bfloat16
                        )
                        active_copy(way, chunk).start()
                        absorb(way, chunk)

            back = at - (stages - 1) - place

            @pl.when(jnp.logical_and(place > 0, jnp.logical_and(back >= 0, back < chunks)))
            def _():
                active_copy(way, back).wait_recv()

                @pl.when(place < stages - 1)
                def _():
                    active_copy(way, back).start()

                absorb(way, back)

        return carry

    def active_copy(way, chunk):
        return remote(
            active.at[way, chunk],
            active.at[way, chunk],
            active_send.at[way, chunk],
            active_recv.at[way, chunk],
            t,
            s + (1 if way == 0 else -1),
        )

    lax.fori_loop(0, chunks + 2 * (stages - 1), slot, 0)

    down_copies = []
    for offset in range(1, ranks):
        rank = lax.rem(t + offset, ranks)
        block = down_total[pl.ds(pl.multiple_of(rank * rows, rows), rows), :]
        down_out[offset - 1] = block.astype(jnp.bfloat16)
        copy = remote(
            down_out.at[offset - 1],
            down_in.at[offset - 1],
            down_send.at[offset - 1],
            down_recv.at[offset - 1],
            rank,
            s,
        )
        copy.start()
        down_copies.append(copy)
    summed = down_total[pl.ds(pl.multiple_of(t * rows, rows), rows), :]
    for offset in range(1, ranks):
        down_copies[offset - 1].wait_recv()
        summed = summed + down_in[offset - 1].astype(jnp.float32)
    last_out[...] = summed.astype(jnp.bfloat16)
    last_copy = remote(last_out, last_in, last_send, last_recv, s, t)

    @pl.when(s != t)
    def _():
        last_copy.start()
        last_copy.wait_recv()

    @pl.when(s == t)
    def _():
        last_in[...] = last_out[...]

    result = mixed[...] + modulation_ref[3:4, :] * last_in[...].astype(jnp.float32)
    result_ref[...] = result.astype(jnp.bfloat16).reshape(result_ref.shape)

    for copy in head_copies + attend_copies + project_copies + sums_copies + down_copies:
        copy.wait_send()
    for offset in range(1, ranks):
        normed_copy(offset).wait_send()

    @pl.when(s != t)
    def _():
        normed_copy(0).wait_send()
        last_copy.wait_send()

    def drain(chunk, carry):
        for way in range(2):
            place = s if way == 0 else stages - 1 - s

            @pl.when(place > 0)
            def _():
                remote(
                    hidden_out.at[way, chunk],
                    hidden_in.at[way, chunk],
                    hidden_send.at[way, chunk],
                    hidden_recv.at[way, chunk],
                    t,
                    s + (-1 if way == 0 else 1),
                ).wait_send()

            @pl.when(place < stages - 1)
            def _():
                active_copy(way, chunk).wait_send()

        return carry

    lax.fori_loop(0, chunks, drain, 0)


def stationary(ranks, stages, *operands):
    query_rows, _, _, residual, _, out_weight, up_weight, down_weight = operands
    members = ranks * stages
    batches, few_tokens, inner = query_rows.shape
    width = inner // members
    tokens = few_tokens * members
    rows = batches * tokens // stages
    half = rows * stages // 2
    features = out_weight.shape[0]
    depth, hidden = up_weight.shape
    band = BAND
    chunks = hidden // band
    bands = (chunks, depth, band)
    half_type, dma = jnp.bfloat16, pltpu.SemaphoreType.DMA
    scratch = [
        pltpu.VMEM(out_weight.shape, half_type),
        pltpu.VMEM(bands, half_type),
        pltpu.VMEM(bands, half_type),
        pltpu.VMEM((3, members, batches, few_tokens, width), half_type),
        pltpu.VMEM((ranks, batches, tokens, width), half_type),
        pltpu.VMEM((batches, tokens, features), jnp.float32),
        pltpu.VMEM((stages - 1, rows, features), half_type),
        pltpu.VMEM((stages - 1, rows, features), half_type),
        pltpu.VMEM((rows, features), jnp.float32),
        pltpu.VMEM((ranks, rows, 128), jnp.float32),
        pltpu.VMEM((rows, features), half_type),
        pltpu.VMEM((2 * half, depth), half_type),
        pltpu.VMEM((2, chunks, half, band), half_type),
        pltpu.VMEM((2, chunks, half, band), half_type),
        pltpu.VMEM((2, chunks, half, band), half_type),
        pltpu.VMEM((2 * half, depth), jnp.float32),
        pltpu.VMEM((ranks - 1, rows, depth), half_type),
        pltpu.VMEM((ranks - 1, rows, depth), half_type),
        pltpu.VMEM((rows, depth), half_type),
        pltpu.VMEM((rows, depth), half_type),
        dma,
        dma((2, chunks)),
        dma((3,)),
        dma((3, members - 1)),
        dma((3, members - 1)),
        dma((batches, ranks - 1)),
        dma((batches, ranks - 1)),
        dma((stages - 1,)),
        dma((stages - 1,)),
        dma((ranks - 1,)),
        dma((ranks - 1,)),
        dma((ranks,)),
        dma((stages,)),
        dma((2, chunks)),
        dma((2, chunks)),
        dma((2, chunks)),
        dma((2, chunks)),
        dma((ranks - 1,)),
        dma((ranks - 1,)),
        dma,
        dma,
    ]
    vmem = pl.BlockSpec(memory_space=pltpu.VMEM)
    return pl.pallas_call(
        functools.partial(block_kernel, ranks, stages, chunks),
        out_shape=jax.ShapeDtypeStruct(residual.shape, half_type),
        in_specs=[vmem] * 5 + [pl.BlockSpec(memory_space=pl.ANY)] * 3,
        out_specs=vmem,
        scratch_shapes=scratch,
        compiler_params=pltpu.CompilerParams(
            collective_id=0, has_side_effects=True, vmem_limit_bytes=40 * 1024 * 1024
        ),
    )(*operands)


def solution(mesh):
    in_specs = (
        P("groups", ("sp", "tp"), None),
        P("groups", ("sp", "tp"), None),
        P("groups", ("sp", "tp"), None),
        P("groups", "sp", "tp"),
        P(None, "tp"),
        P("tp", "sp"),
        P("sp", "tp"),
        P("sp", "tp"),
    )
    out_specs = P("groups", "sp", "tp")
    def block(*operands):
        sizes = mesh.shape
        rows = operands[0].shape[0] * operands[0].shape[1] * sizes["sp"] * sizes["tp"]
        square = sizes["sp"] == sizes["tp"]
        whole_heads = operands[0].shape[2] % (sizes["sp"] * sizes["tp"] * HEAD_FEATURES) == 0
        few = operands[6].shape[1] % BAND == 0 and rows < operands[6].shape[0]
        if square and whole_heads and few:
            return stationary(sizes["tp"], sizes["sp"], *operands)
        return body(*operands)

    return jax.shard_map(block, mesh=mesh, in_specs=in_specs, out_specs=out_specs, check_vma=False)
```

```python
import functools
import math

import jax
import jax.numpy as jnp
from jax import lax
from jax.experimental import pallas as pl
from jax.experimental.pallas import tpu as pltpu
from jax.sharding import PartitionSpec as P

D = 2560
HEAD_FEATURES = 128
BAND = 256


def contract_last(left, right):
    return lax.dot_general(
        left, right, (((1,), (1,)), ((), ())), preferred_element_type=jnp.float32
    )


def attend(query_part, key_part, value_part):
    query_heads, key_heads, value_heads = (
        lax.all_to_all(query_part, "sp", split_axis=2, concat_axis=1, tiled=True),
        lax.all_to_all(key_part, "sp", split_axis=2, concat_axis=1, tiled=True),
        lax.all_to_all(value_part, "sp", split_axis=2, concat_axis=1, tiled=True),
    )
    batches, query_count, local_width = query_heads.shape
    local_heads = local_width // HEAD_FEATURES
    grouped = query_heads.reshape(batches, query_count, local_heads, HEAD_FEATURES)
    score_scale = 1.0 / math.sqrt(HEAD_FEATURES)

    def absorb_block(running, blocks):
        block_keys, block_values = blocks
        highest, row_total, weighted_values = running
        attention_logits = (
            jnp.einsum("bqhd,bkhd->bqhk", grouped, block_keys, preferred_element_type=jnp.float32)
            * score_scale
        )
        raised = jnp.maximum(highest, jnp.max(attention_logits, axis=-1))
        damping = jnp.exp(highest - raised)
        exponent = jnp.exp(attention_logits - raised[..., None])
        row_total = row_total * damping + jnp.sum(exponent, axis=-1)
        weighted_values = weighted_values * damping[..., None] + jnp.einsum(
            "bqhk,bkhd->bqhd",
            exponent.astype(jnp.bfloat16),
            block_values,
            preferred_element_type=jnp.float32,
        )
        return (raised, row_total, weighted_values)

    def scan_step(running, blocks):
        return (absorb_block(running, blocks), None)

    def absorb(running, section):
        key_section, value_section = section
        key_count = key_section.shape[1]
        shaped_keys = key_section.reshape(batches, key_count, local_heads, HEAD_FEATURES)
        shaped_values = value_section.reshape(batches, key_count, local_heads, HEAD_FEATURES)
        if key_count > 512 and key_count % 512 == 0:
            block_count = key_count // 512
            key_blocks = jnp.moveaxis(
                shaped_keys.reshape(batches, block_count, 512, local_heads, HEAD_FEATURES), 1, 0
            )
            value_blocks = jnp.moveaxis(
                shaped_values.reshape(batches, block_count, 512, local_heads, HEAD_FEATURES), 1, 0
            )
            running, unused = lax.scan(scan_step, running, (key_blocks, value_blocks))
            return running
        return absorb_block(running, (shaped_keys, shaped_values))

    starting = (
        jnp.full((batches, query_count, local_heads), -jnp.inf, jnp.float32),
        jnp.zeros((batches, query_count, local_heads), jnp.float32),
        jnp.zeros((batches, query_count, local_heads, HEAD_FEATURES), jnp.float32),
    )
    highest, row_total, weighted_values = absorb(
        starting,
        (
            lax.all_gather(key_heads, "tp", axis=1, tiled=True),
            lax.all_gather(value_heads, "tp", axis=1, tiled=True),
        ),
    )
    normalized = (weighted_values / row_total[..., None]).astype(jnp.bfloat16)
    ordered = normalized.reshape(batches, query_count, local_width)
    return lax.all_to_all(ordered, "sp", split_axis=1, concat_axis=2, tiled=True)


def body(
    query_rows, key_rows, value_rows, residual, modulation, out_weight, up_weight, down_weight
):
    attended = attend(query_rows, key_rows, value_rows)
    stripes = lax.all_gather(attended, "tp", axis=1, tiled=True)
    batches, rows_block, inner_width = stripes.shape
    row_count = batches * rows_block
    flat_rows = stripes.reshape(row_count, inner_width)
    local_width = out_weight.shape[0]
    columns = flat_rows
    projected = contract_last(columns, lax.all_gather(out_weight, "sp", axis=1, tiled=True))
    mixed_rows = (
        residual.reshape(row_count, local_width).astype(jnp.float32) + modulation[0] * projected
    )
    first_sum, second_sum = lax.psum(
        (jnp.sum(mixed_rows, axis=1), jnp.sum(mixed_rows * mixed_rows, axis=1)), "tp"
    )
    row_mean = first_sum / D
    spread = second_sum / D - row_mean * row_mean
    normed = (
        (mixed_rows - row_mean[:, None])
        * lax.rsqrt(spread[:, None] + 1e-06)
        * (1.0 + modulation[2])
        + modulation[1]
    ).astype(jnp.bfloat16)
    gathered = lax.all_gather(normed, "tp", axis=1, tiled=True)
    columns = gathered
    hidden = jnp.dot(
        columns,
        lax.all_gather(up_weight, "sp", axis=0, tiled=True),
        preferred_element_type=jnp.float32,
    )
    active = jax.nn.gelu(hidden, approximate=True).astype(jnp.bfloat16)
    partial_out = contract_last(active, lax.all_gather(down_weight, "sp", axis=0, tiled=True))
    summed = lax.psum_scatter(
        partial_out.astype(jnp.bfloat16), "tp", scatter_dimension=1, tiled=True
    ).astype(jnp.float32)
    result = (mixed_rows + modulation[3] * summed).astype(jnp.bfloat16)
    return result.reshape(batches, rows_block, local_width)


def block_kernel(
    ranks,
    stages,
    chunks,
    query_hbm,
    key_hbm,
    value_hbm,
    residual_hbm,
    modulation_hbm,
    out_hbm,
    up_hbm,
    down_hbm,
    result_ref,
    query_ref,
    key_ref,
    value_ref,
    residual_ref,
    modulation_ref,
    out_weight,
    up_weight,
    down_weight,
    heads,
    attended,
    projected,
    outgoing,
    incoming,
    mixed,
    sums,
    normed_out,
    normed,
    hidden_out,
    hidden_in,
    active,
    down_total,
    down_out,
    down_in,
    last_out,
    last_in,
    input_sem,
    out_sem,
    weight_sem,
    own_sem,
    head_send,
    head_recv,
    attend_send,
    attend_recv,
    project_send,
    project_recv,
    sums_send,
    sums_recv,
    normed_send,
    normed_recv,
    relay_send,
    hidden_send,
    hidden_recv,
    active_send,
    active_recv,
    down_send,
    down_recv,
    last_send,
    last_recv,
):
    t, s = lax.axis_index("tp"), lax.axis_index("sp")
    members = ranks * stages
    me = s * ranks + t
    core = lax.rem(t, 2)
    chip = lax.div(t, 2)
    chips = ranks // 2
    sibling = t + 1 - 2 * core
    batches, few_tokens, _ = query_ref.shape
    width = heads.shape[-1]
    tokens = members * few_tokens
    part = tokens // stages
    rows = batches * part
    half = rows * stages // 2
    band = hidden_in.shape[-1]

    def remote(source, target, send, recv, rank, stage):
        return pltpu.make_async_remote_copy(
            src_ref=source,
            dst_ref=target,
            send_sem=send,
            recv_sem=recv,
            device_id={"tp": rank, "sp": stage},
            device_id_type=pl.DeviceIdType.MESH,
        )

    input_copies = [
        pltpu.make_async_copy(source, target, input_sem.at[at])
        for at, (source, target) in enumerate(
            (
                (query_hbm, query_ref),
                (key_hbm, key_ref),
                (value_hbm, value_ref),
                (residual_hbm, residual_ref),
                (modulation_hbm, modulation_ref),
            )
        )
    ]
    for copy in input_copies:
        copy.start()
    out_copy = pltpu.make_async_copy(out_hbm, out_weight, out_sem)
    up_copies, down_copies_in = (
        [
            pltpu.make_async_copy(
                source.at[:, chunk * band : (chunk + 1) * band],
                target.at[chunk],
                weight_sem.at[at, chunk],
            )
            for chunk in range(chunks)
        ]
        for at, (source, target) in enumerate(((up_hbm, up_weight), (down_hbm, down_weight)))
    )
    for copy in [out_copy, *up_copies, *down_copies_in]:
        copy.start()

    barrier = pltpu.get_barrier_semaphore()
    for offset in range(1, members):
        other = lax.rem(me + offset, members)
        pl.semaphore_signal(
            barrier,
            inc=1,
            device_id={"tp": lax.rem(other, ranks), "sp": lax.div(other, ranks)},
            device_id_type=pl.DeviceIdType.MESH,
        )
    for copy in input_copies:
        copy.wait()
    pl.semaphore_wait(barrier, members - 1)

    def head_copy(at, source, offset):
        other = lax.rem(me + offset, members)
        columns = pl.ds(pl.multiple_of(other * width, width), width)
        return remote(
            source.at[:, :, columns],
            heads.at[at, me],
            head_send.at[at, offset - 1],
            head_recv.at[at, offset - 1],
            lax.rem(other, ranks),
            lax.div(other, ranks),
        )

    sources = (query_ref, key_ref, value_ref)
    head_copies = [
        head_copy(at, source, offset)
        for offset in range(1, members)
        for at, source in enumerate(sources)
    ]
    for copy in head_copies:
        copy.start()
    own_columns = pl.ds(pl.multiple_of(me * width, width), width)
    own_copies = [
        pltpu.make_async_copy(source.at[:, :, own_columns], heads.at[at, me], own_sem.at[at])
        for at, source in enumerate(sources)
    ]
    for copy in own_copies:
        copy.start()
    for copy in own_copies:
        copy.wait()
    for copy in head_copies:
        copy.wait_recv()

    def head_rows(at, batch, columns):
        loaded = heads[at, :, batch, :, columns].astype(jnp.float32)
        return loaded.reshape(tokens, HEAD_FEATURES).astype(jnp.bfloat16)

    score_scale = 1.0 / math.sqrt(HEAD_FEATURES)
    def attend_copy(batch, source, at, rank):
        return remote(
            attended.at[source, batch],
            attended.at[source, batch],
            attend_send.at[batch, at],
            attend_recv.at[batch, source],
            rank,
            s,
        )

    attend_copies = []
    for batch in range(batches):
        for head in range(width // HEAD_FEATURES):
            columns = slice(head * HEAD_FEATURES, (head + 1) * HEAD_FEATURES)
            scores = score_scale * contract_last(
                head_rows(0, batch, columns), head_rows(1, batch, columns)
            )
            exponent = jnp.exp(scores - jnp.max(scores, axis=-1, keepdims=True))
            row_total = jnp.sum(exponent, axis=-1, keepdims=True)
            weighted = jnp.dot(
                exponent.astype(jnp.bfloat16),
                head_rows(2, batch, columns),
                preferred_element_type=jnp.float32,
            )
            attended[t, batch, :, columns] = (weighted / row_total).astype(jnp.bfloat16)
        for offset in range(chips):
            rank = lax.rem(t + 2 * offset, ranks) if offset else sibling
            copy = attend_copy(batch, t, offset, rank)
            copy.start()
            attend_copies.append(copy)

    out_copy.wait()
    for batch in range(batches):
        for offset in range(1, chips):
            source = lax.rem(t + ranks - 2 * offset, ranks)
            copy = attend_copy(batch, source, chips - 1 + offset, sibling)
            copy.wait_recv()
            copy.start()
            attend_copies.append(copy)
    for batch in range(batches):
        for offset in range(chips):
            source = lax.rem(sibling + ranks - 2 * offset, ranks)
            attend_copy(batch, source, 0, sibling).wait_recv()
    total = None
    for rank in range(ranks):
        left = attended[rank].reshape(batches * tokens, width)
        product = contract_last(left, out_weight[:, rank * width : (rank + 1) * width])
        total = product if total is None else total + product
    projected[...] = total.reshape(projected.shape)

    project_copies = []
    for offset in range(1, stages):
        stage = lax.rem(s + offset, stages)
        block = projected[:, pl.ds(pl.multiple_of(stage * part, part), part), :]
        outgoing[offset - 1] = block.reshape(rows, -1).astype(jnp.bfloat16)
        copy = remote(
            outgoing.at[offset - 1],
            incoming.at[offset - 1],
            project_send.at[offset - 1],
            project_recv.at[offset - 1],
            t,
            stage,
        )
        copy.start()
        project_copies.append(copy)
    kept = projected[:, pl.ds(pl.multiple_of(s * part, part), part), :].reshape(rows, -1)
    for offset in range(1, stages):
        project_copies[offset - 1].wait_recv()
        kept = kept + incoming[offset - 1].astype(jnp.float32)
    stream = residual_ref[...].astype(jnp.float32).reshape(rows, -1)
    stream = stream + modulation_ref[0:1, :] * kept
    mixed[...] = stream
    first = jnp.sum(stream, axis=1, keepdims=True)
    second = jnp.sum(stream * stream, axis=1, keepdims=True)
    lanes = lax.broadcasted_iota(jnp.int32, (rows, 128), 1)
    sums[t] = jnp.where(lanes == 0, first, second)
    sums_copies = []
    for offset in range(1, ranks):
        copy = remote(
            sums.at[t],
            sums.at[t],
            sums_send.at[offset - 1],
            sums_recv.at[offset - 1],
            lax.rem(t + offset, ranks),
            s,
        )
        copy.start()
        sums_copies.append(copy)
    for copy in sums_copies:
        copy.wait_recv()
    both_sums = sums[0]
    for rank in range(1, ranks):
        both_sums = both_sums + sums[rank]
    row_mean = both_sums[:, 0:1] / D
    spread = both_sums[:, 1:2] / D - row_mean * row_mean
    normed_rows = (
        (mixed[...] - row_mean)
        * lax.rsqrt(spread + 1e-06)
        * (1.0 + modulation_ref[2:3, :])
        + modulation_ref[1:2, :]
    ).astype(jnp.bfloat16)
    normed_out[...] = normed_rows

    own_rows = pl.ds(pl.multiple_of(s * rows, rows), rows)
    own_core = lax.rem(s, 2)

    def normed_copy(offset):
        return remote(
            normed_out,
            normed.at[own_rows],
            normed_send.at[offset],
            normed_recv.at[s],
            2 * lax.rem(chip + offset, chips) + own_core,
            t,
        )

    def relay_copy(at, source):
        block = normed.at[pl.ds(pl.multiple_of(source * rows, rows), rows)]
        return remote(block, block, relay_send.at[at], normed_recv.at[source], sibling, s)

    for offset in range(1, chips):
        normed_copy(offset).start()

    @pl.when(s != t)
    def _():
        normed_copy(0).start()

    @pl.when(s == t)
    def _():
        normed[own_rows, :] = normed_rows

    relays = [relay_copy(at, 2 * at + core) for at in range(stages // 2)]
    for at, relay in enumerate(relays):

        @pl.when(jnp.logical_or(t != s, s != 2 * at + core))
        def _():
            relay.wait_recv()

        relay.start()
    for at in range(stages // 2):
        relay_copy(at, 2 * at + 1 - core).wait_recv()
    for copy in up_copies:
        copy.wait()
    for copy in down_copies_in:
        copy.wait()
    down_total[...] = jnp.zeros_like(down_total)

    def absorb(way, chunk):
        block = contract_last(active[way, chunk], down_weight[chunk])
        down_total[way * half : (way + 1) * half, :] += block

    def slot(at, carry):
        for way in range(2):
            place = s if way == 0 else stages - 1 - s
            toward = -1 if way == 0 else 1
            chunk = at - (stages - 1 - place)

            @pl.when(jnp.logical_and(chunk >= 0, chunk < chunks))
            def _():
                partial = jnp.dot(
                    normed[way * half : (way + 1) * half, :],
                    up_weight[chunk],
                    preferred_element_type=jnp.float32,
                )
                hidden_out[way, chunk] = partial.astype(jnp.bfloat16)

                def hidden_copy():
                    return remote(
                        hidden_out.at[way, chunk],
                        hidden_in.at[way, chunk],
                        hidden_send.at[way, chunk],
                        hidden_recv.at[way, chunk],
                        t,
                        s + toward,
                    )

                @pl.when(place == stages - 1)
                def _():
                    hidden_copy().start()

                @pl.when(place < stages - 1)
                def _():
                    hidden_copy().wait_recv()
                    combined = partial + hidden_in[way, chunk].astype(jnp.float32)

                    @pl.when(place > 0)
                    def _():
                        hidden_out[way, chunk] = combined.astype(jnp.bfloat16)
                        hidden_copy().start()

                    @pl.when(place == 0)
                    def _():
                        active[way, chunk] = jax.nn.gelu(combined, approximate=True).astype(
                            jnp.bfloat16
                        )
                        active_copy(way, chunk).start()
                        absorb(way, chunk)

            back = at - (stages - 1) - place

            @pl.when(jnp.logical_and(place > 0, jnp.logical_and(back >= 0, back < chunks)))
            def _():
                active_copy(way, back).wait_recv()

                @pl.when(place < stages - 1)
                def _():
                    active_copy(way, back).start()

                absorb(way, back)

        return carry

    def active_copy(way, chunk):
        return remote(
            active.at[way, chunk],
            active.at[way, chunk],
            active_send.at[way, chunk],
            active_recv.at[way, chunk],
            t,
            s + (1 if way == 0 else -1),
        )

    lax.fori_loop(0, chunks + 2 * (stages - 1), slot, 0)

    down_copies = []
    for offset in range(1, ranks):
        rank = lax.rem(t + offset, ranks)
        block = down_total[pl.ds(pl.multiple_of(rank * rows, rows), rows), :]
        down_out[offset - 1] = block.astype(jnp.bfloat16)
        copy = remote(
            down_out.at[offset - 1],
            down_in.at[offset - 1],
            down_send.at[offset - 1],
            down_recv.at[offset - 1],
            rank,
            s,
        )
        copy.start()
        down_copies.append(copy)
    summed = down_total[pl.ds(pl.multiple_of(t * rows, rows), rows), :]
    for offset in range(1, ranks):
        down_copies[offset - 1].wait_recv()
        summed = summed + down_in[offset - 1].astype(jnp.float32)
    last_out[...] = summed.astype(jnp.bfloat16)
    last_copy = remote(last_out, last_in, last_send, last_recv, s, t)

    @pl.when(s != t)
    def _():
        last_copy.start()
        last_copy.wait_recv()

    @pl.when(s == t)
    def _():
        last_in[...] = last_out[...]

    result = mixed[...] + modulation_ref[3:4, :] * last_in[...].astype(jnp.float32)
    result_ref[...] = result.astype(jnp.bfloat16).reshape(result_ref.shape)

    for copy in head_copies + attend_copies + project_copies + sums_copies + down_copies:
        copy.wait_send()
    for offset in range(1, chips):
        normed_copy(offset).wait_send()
    for relay in relays:
        relay.wait_send()

    @pl.when(s != t)
    def _():
        normed_copy(0).wait_send()
        last_copy.wait_send()

    def drain(chunk, carry):
        for way in range(2):
            place = s if way == 0 else stages - 1 - s

            @pl.when(place > 0)
            def _():
                remote(
                    hidden_out.at[way, chunk],
                    hidden_in.at[way, chunk],
                    hidden_send.at[way, chunk],
                    hidden_recv.at[way, chunk],
                    t,
                    s + (-1 if way == 0 else 1),
                ).wait_send()

            @pl.when(place < stages - 1)
            def _():
                active_copy(way, chunk).wait_send()

        return carry

    lax.fori_loop(0, chunks, drain, 0)


def stationary(ranks, stages, *operands):
    query_rows, _, _, residual, _, out_weight, up_weight, down_weight = operands
    members = ranks * stages
    batches, few_tokens, inner = query_rows.shape
    width = inner // members
    tokens = few_tokens * members
    rows = batches * tokens // stages
    half = rows * stages // 2
    features = out_weight.shape[0]
    depth, hidden = up_weight.shape
    band = BAND
    chunks = hidden // band
    bands = (chunks, depth, band)
    half_type, dma = jnp.bfloat16, pltpu.SemaphoreType.DMA
    scratch = [
        *(pltpu.VMEM(operand.shape, operand.dtype) for operand in operands[:5]),
        pltpu.VMEM(out_weight.shape, half_type),
        pltpu.VMEM(bands, half_type),
        pltpu.VMEM(bands, half_type),
        pltpu.VMEM((3, members, batches, few_tokens, width), half_type),
        pltpu.VMEM((ranks, batches, tokens, width), half_type),
        pltpu.VMEM((batches, tokens, features), jnp.float32),
        pltpu.VMEM((stages - 1, rows, features), half_type),
        pltpu.VMEM((stages - 1, rows, features), half_type),
        pltpu.VMEM((rows, features), jnp.float32),
        pltpu.VMEM((ranks, rows, 128), jnp.float32),
        pltpu.VMEM((rows, features), half_type),
        pltpu.VMEM((2 * half, depth), half_type),
        pltpu.VMEM((2, chunks, half, band), half_type),
        pltpu.VMEM((2, chunks, half, band), half_type),
        pltpu.VMEM((2, chunks, half, band), half_type),
        pltpu.VMEM((2 * half, depth), jnp.float32),
        pltpu.VMEM((ranks - 1, rows, depth), half_type),
        pltpu.VMEM((ranks - 1, rows, depth), half_type),
        pltpu.VMEM((rows, depth), half_type),
        pltpu.VMEM((rows, depth), half_type),
        dma((5,)),
        dma,
        dma((2, chunks)),
        dma((3,)),
        dma((3, members - 1)),
        dma((3, members - 1)),
        dma((batches, ranks - 1)),
        dma((batches, ranks)),
        dma((stages - 1,)),
        dma((stages - 1,)),
        dma((ranks - 1,)),
        dma((ranks - 1,)),
        dma((ranks // 2,)),
        dma((stages,)),
        dma((stages // 2,)),
        dma((2, chunks)),
        dma((2, chunks)),
        dma((2, chunks)),
        dma((2, chunks)),
        dma((ranks - 1,)),
        dma((ranks - 1,)),
        dma,
        dma,
    ]
    vmem = pl.BlockSpec(memory_space=pltpu.VMEM)
    return pl.pallas_call(
        functools.partial(block_kernel, ranks, stages, chunks),
        out_shape=jax.ShapeDtypeStruct(residual.shape, half_type),
        in_specs=[pl.BlockSpec(memory_space=pl.ANY)] * 8,
        out_specs=vmem,
        scratch_shapes=scratch,
        compiler_params=pltpu.CompilerParams(
            collective_id=0, has_side_effects=True, vmem_limit_bytes=62 * 1024 * 1024
        ),
    )(*operands)


def solution(mesh):
    in_specs = (
        P("groups", ("sp", "tp"), None),
        P("groups", ("sp", "tp"), None),
        P("groups", ("sp", "tp"), None),
        P("groups", "sp", "tp"),
        P(None, "tp"),
        P("tp", "sp"),
        P("sp", "tp"),
        P("sp", "tp"),
    )
    out_specs = P("groups", "sp", "tp")
    def block(*operands):
        sizes = mesh.shape
        rows = operands[0].shape[0] * operands[0].shape[1] * sizes["sp"] * sizes["tp"]
        square = sizes["sp"] == sizes["tp"] and sizes["sp"] % 2 == 0
        whole_heads = operands[0].shape[2] % (sizes["sp"] * sizes["tp"] * HEAD_FEATURES) == 0
        few = operands[6].shape[1] % BAND == 0 and rows < operands[6].shape[0]
        if square and whole_heads and few:
            return stationary(sizes["tp"], sizes["sp"], *operands)
        return body(*operands)

    return jax.shard_map(block, mesh=mesh, in_specs=in_specs, out_specs=out_specs, check_vma=False)
```

```python
import functools
import math

import jax
import jax.numpy as jnp
from jax import lax
from jax.experimental import pallas as pl
from jax.experimental.pallas import tpu as pltpu
from jax.sharding import PartitionSpec as P

D = 2560
HEAD_FEATURES = 128
BAND = 128
LAG = 5


def contract_last(left, right):
    return lax.dot_general(
        left, right, (((1,), (1,)), ((), ())), preferred_element_type=jnp.float32
    )


def attend(query_part, key_part, value_part):
    query_heads, key_heads, value_heads = (
        lax.all_to_all(query_part, "sp", split_axis=2, concat_axis=1, tiled=True),
        lax.all_to_all(key_part, "sp", split_axis=2, concat_axis=1, tiled=True),
        lax.all_to_all(value_part, "sp", split_axis=2, concat_axis=1, tiled=True),
    )
    batches, query_count, local_width = query_heads.shape
    local_heads = local_width // HEAD_FEATURES
    grouped = query_heads.reshape(batches, query_count, local_heads, HEAD_FEATURES)
    score_scale = 1.0 / math.sqrt(HEAD_FEATURES)

    def absorb_block(running, blocks):
        block_keys, block_values = blocks
        highest, row_total, weighted_values = running
        attention_logits = (
            jnp.einsum("bqhd,bkhd->bqhk", grouped, block_keys, preferred_element_type=jnp.float32)
            * score_scale
        )
        raised = jnp.maximum(highest, jnp.max(attention_logits, axis=-1))
        damping = jnp.exp(highest - raised)
        exponent = jnp.exp(attention_logits - raised[..., None])
        row_total = row_total * damping + jnp.sum(exponent, axis=-1)
        weighted_values = weighted_values * damping[..., None] + jnp.einsum(
            "bqhk,bkhd->bqhd",
            exponent.astype(jnp.bfloat16),
            block_values,
            preferred_element_type=jnp.float32,
        )
        return (raised, row_total, weighted_values)

    def scan_step(running, blocks):
        return (absorb_block(running, blocks), None)

    def absorb(running, section):
        key_section, value_section = section
        key_count = key_section.shape[1]
        shaped_keys = key_section.reshape(batches, key_count, local_heads, HEAD_FEATURES)
        shaped_values = value_section.reshape(batches, key_count, local_heads, HEAD_FEATURES)
        if key_count > 512 and key_count % 512 == 0:
            block_count = key_count // 512
            key_blocks = jnp.moveaxis(
                shaped_keys.reshape(batches, block_count, 512, local_heads, HEAD_FEATURES), 1, 0
            )
            value_blocks = jnp.moveaxis(
                shaped_values.reshape(batches, block_count, 512, local_heads, HEAD_FEATURES), 1, 0
            )
            running, unused = lax.scan(scan_step, running, (key_blocks, value_blocks))
            return running
        return absorb_block(running, (shaped_keys, shaped_values))

    starting = (
        jnp.full((batches, query_count, local_heads), -jnp.inf, jnp.float32),
        jnp.zeros((batches, query_count, local_heads), jnp.float32),
        jnp.zeros((batches, query_count, local_heads, HEAD_FEATURES), jnp.float32),
    )
    highest, row_total, weighted_values = absorb(
        starting,
        (
            lax.all_gather(key_heads, "tp", axis=1, tiled=True),
            lax.all_gather(value_heads, "tp", axis=1, tiled=True),
        ),
    )
    normalized = (weighted_values / row_total[..., None]).astype(jnp.bfloat16)
    ordered = normalized.reshape(batches, query_count, local_width)
    return lax.all_to_all(ordered, "sp", split_axis=1, concat_axis=2, tiled=True)


def body(
    query_rows, key_rows, value_rows, residual, modulation, out_weight, up_weight, down_weight
):
    attended = attend(query_rows, key_rows, value_rows)
    stripes = lax.all_gather(attended, "tp", axis=1, tiled=True)
    batches, rows_block, inner_width = stripes.shape
    row_count = batches * rows_block
    flat_rows = stripes.reshape(row_count, inner_width)
    local_width = out_weight.shape[0]
    columns = flat_rows
    projected = contract_last(columns, lax.all_gather(out_weight, "sp", axis=1, tiled=True))
    mixed_rows = (
        residual.reshape(row_count, local_width).astype(jnp.float32) + modulation[0] * projected
    )
    first_sum, second_sum = lax.psum(
        (jnp.sum(mixed_rows, axis=1), jnp.sum(mixed_rows * mixed_rows, axis=1)), "tp"
    )
    row_mean = first_sum / D
    spread = second_sum / D - row_mean * row_mean
    normed = (
        (mixed_rows - row_mean[:, None])
        * lax.rsqrt(spread[:, None] + 1e-06)
        * (1.0 + modulation[2])
        + modulation[1]
    ).astype(jnp.bfloat16)
    gathered = lax.all_gather(normed, "tp", axis=1, tiled=True)
    columns = gathered
    hidden = jnp.dot(
        columns,
        lax.all_gather(up_weight, "sp", axis=0, tiled=True),
        preferred_element_type=jnp.float32,
    )
    active = jax.nn.gelu(hidden, approximate=True).astype(jnp.bfloat16)
    partial_out = contract_last(active, lax.all_gather(down_weight, "sp", axis=0, tiled=True))
    summed = lax.psum_scatter(
        partial_out.astype(jnp.bfloat16), "tp", scatter_dimension=1, tiled=True
    ).astype(jnp.float32)
    result = (mixed_rows + modulation[3] * summed).astype(jnp.bfloat16)
    return result.reshape(batches, rows_block, local_width)


def block_kernel(
    ranks,
    stages,
    chunks,
    query_hbm,
    key_hbm,
    value_hbm,
    residual_hbm,
    modulation_hbm,
    out_hbm,
    up_hbm,
    down_hbm,
    result_ref,
    query_ref,
    key_ref,
    value_ref,
    residual_ref,
    modulation_ref,
    out_weight,
    up_weight,
    down_weight,
    heads,
    attended,
    projected,
    outgoing,
    incoming,
    mixed,
    sums,
    normed_out,
    normed,
    hidden_own,
    hidden_out,
    hidden_in,
    active,
    down_total,
    down_out,
    down_in,
    last_out,
    last_in,
    input_sem,
    out_sem,
    weight_sem,
    own_sem,
    head_send,
    head_recv,
    attend_send,
    attend_recv,
    project_send,
    project_recv,
    sums_send,
    sums_recv,
    normed_send,
    normed_recv,
    relay_send,
    hidden_send,
    hidden_recv,
    active_send,
    active_recv,
    down_send,
    down_recv,
    last_send,
    last_recv,
):
    t, s = lax.axis_index("tp"), lax.axis_index("sp")
    members = ranks * stages
    me = s * ranks + t
    core = lax.rem(t, 2)
    chip = lax.div(t, 2)
    chips = ranks // 2
    sibling = t + 1 - 2 * core
    batches, few_tokens, _ = query_ref.shape
    width = heads.shape[-1]
    tokens = members * few_tokens
    part = tokens // stages
    rows = batches * part
    half = tokens
    band = hidden_in.shape[-1]

    def remote(source, target, send, recv, rank, stage):
        return pltpu.make_async_remote_copy(
            src_ref=source,
            dst_ref=target,
            send_sem=send,
            recv_sem=recv,
            device_id={"tp": rank, "sp": stage},
            device_id_type=pl.DeviceIdType.MESH,
        )

    input_copies = [
        pltpu.make_async_copy(source, target, input_sem.at[at])
        for at, (source, target) in enumerate(
            (
                (query_hbm, query_ref),
                (key_hbm, key_ref),
                (value_hbm, value_ref),
                (residual_hbm, residual_ref),
                (modulation_hbm, modulation_ref),
            )
        )
    ]
    for copy in input_copies:
        copy.start()
    out_copy = pltpu.make_async_copy(out_hbm, out_weight, out_sem)
    up_copies, down_copies_in = (
        [
            pltpu.make_async_copy(
                source.at[:, chunk * band : (chunk + 1) * band],
                target.at[chunk],
                weight_sem.at[at, chunk],
            )
            for chunk in range(chunks)
        ]
        for at, (source, target) in enumerate(((up_hbm, up_weight), (down_hbm, down_weight)))
    )
    for copy in [out_copy, *up_copies, *down_copies_in]:
        copy.start()

    barrier = pltpu.get_barrier_semaphore()
    for offset in range(1, members):
        other = lax.rem(me + offset, members)
        pl.semaphore_signal(
            barrier,
            inc=1,
            device_id={"tp": lax.rem(other, ranks), "sp": lax.div(other, ranks)},
            device_id_type=pl.DeviceIdType.MESH,
        )
    for copy in input_copies:
        copy.wait()
    pl.semaphore_wait(barrier, members - 1)

    def head_copy(batch, at, source, offset):
        other = lax.rem(me + offset, members)
        columns = pl.ds(pl.multiple_of(other * width, width), width)
        return remote(
            source.at[batch, :, columns],
            heads.at[at, batch, me],
            head_send.at[batch, at, offset - 1],
            head_recv.at[batch, at, offset - 1],
            lax.rem(other, ranks),
            lax.div(other, ranks),
        )

    sources = (query_ref, key_ref, value_ref)
    head_copies = [
        [
            head_copy(batch, at, source, offset)
            for offset in range(1, members)
            for at, source in enumerate(sources)
        ]
        for batch in range(batches)
    ]
    own_columns = pl.ds(pl.multiple_of(me * width, width), width)
    own_copies = [
        pltpu.make_async_copy(
            source.at[batch, :, own_columns], heads.at[at, batch, me], own_sem.at[batch, at]
        )
        for batch in range(batches)
        for at, source in enumerate(sources)
    ]
    for copy in head_copies[0] + head_copies[1] + own_copies:
        copy.start()
    for copy in own_copies:
        copy.wait()

    def head_rows(at, batch, columns):
        loaded = heads[at, batch, :, :, columns].astype(jnp.float32)
        return loaded.reshape(tokens, HEAD_FEATURES).astype(jnp.bfloat16)

    score_scale = 1.0 / math.sqrt(HEAD_FEATURES)
    def attend_copy(batch, source, at, rank):
        return remote(
            attended.at[source, batch],
            attended.at[source, batch],
            attend_send.at[batch, at],
            attend_recv.at[batch, source],
            rank,
            s,
        )

    attend_copies = []
    for batch in range(batches):
        for copy in head_copies[batch]:
            copy.wait_recv()
        for head in range(width // HEAD_FEATURES):
            columns = slice(head * HEAD_FEATURES, (head + 1) * HEAD_FEATURES)
            scores = score_scale * contract_last(
                head_rows(0, batch, columns), head_rows(1, batch, columns)
            )
            exponent = jnp.exp(scores - jnp.max(scores, axis=-1, keepdims=True))
            row_total = jnp.sum(exponent, axis=-1, keepdims=True)
            weighted = jnp.dot(
                exponent.astype(jnp.bfloat16),
                head_rows(2, batch, columns),
                preferred_element_type=jnp.float32,
            )
            attended[t, batch, :, columns] = (weighted / row_total).astype(jnp.bfloat16)
        for offset in range(chips):
            rank = lax.rem(t + 2 * offset, ranks) if offset else sibling
            copy = attend_copy(batch, t, offset, rank)
            copy.start()
            attend_copies.append(copy)

    out_copy.wait()
    project_copies = []
    for batch in range(batches):
        for offset in range(1, chips):
            source = lax.rem(t + ranks - 2 * offset, ranks)
            copy = attend_copy(batch, source, chips - 1 + offset, sibling)
            copy.wait_recv()
            copy.start()
            attend_copies.append(copy)
        for offset in range(chips):
            source = lax.rem(sibling + ranks - 2 * offset, ranks)
            attend_copy(batch, source, 0, sibling).wait_recv()
        total = None
        for rank in range(ranks):
            columns = slice(rank * width, (rank + 1) * width)
            product = contract_last(attended[rank, batch], out_weight[:, columns])
            total = product if total is None else total + product
        projected[batch] = total
        for offset in range(1, stages):
            stage = lax.rem(s + offset, stages)
            block = projected[batch, pl.ds(pl.multiple_of(stage * part, part), part), :]
            outgoing[batch, offset - 1] = block.astype(jnp.bfloat16)
            copy = remote(
                outgoing.at[batch, offset - 1],
                incoming.at[batch, offset - 1],
                project_send.at[batch, offset - 1],
                project_recv.at[batch, offset - 1],
                t,
                stage,
            )
            copy.start()
            project_copies.append(copy)

    sums_copies = []
    lanes = lax.broadcasted_iota(jnp.int32, (part, 128), 1)
    for batch in range(batches):
        kept = projected[batch, pl.ds(pl.multiple_of(s * part, part), part), :]
        for offset in range(1, stages):
            project_copies[batch * (stages - 1) + offset - 1].wait_recv()
            kept = kept + incoming[batch, offset - 1].astype(jnp.float32)
        stream = residual_ref[batch].astype(jnp.float32) + modulation_ref[0:1, :] * kept
        mixed[batch] = stream
        first = jnp.sum(stream, axis=1, keepdims=True)
        second = jnp.sum(stream * stream, axis=1, keepdims=True)
        sums[batch, t] = jnp.where(lanes == 0, first, second)
        for offset in range(1, ranks):
            copy = remote(
                sums.at[batch, t],
                sums.at[batch, t],
                sums_send.at[batch, offset - 1],
                sums_recv.at[batch, offset - 1],
                lax.rem(t + offset, ranks),
                s,
            )
            copy.start()
            sums_copies.append(copy)

    own_core = lax.rem(s, 2)

    def normed_copy(batch, offset):
        return remote(
            normed_out.at[batch],
            normed.at[batch, s],
            normed_send.at[batch, offset],
            normed_recv.at[batch, s],
            2 * lax.rem(chip + offset, chips) + own_core,
            t,
        )

    def relay_copy(batch, at, source):
        block = normed.at[batch, source]
        return remote(
            block, block, relay_send.at[batch, at], normed_recv.at[batch, source], sibling, s
        )

    for batch in range(batches):
        for copy in sums_copies[batch * (ranks - 1) : (batch + 1) * (ranks - 1)]:
            copy.wait_recv()
        both_sums = sums[batch, 0]
        for rank in range(1, ranks):
            both_sums = both_sums + sums[batch, rank]
        row_mean = both_sums[:, 0:1] / D
        spread = both_sums[:, 1:2] / D - row_mean * row_mean
        normed_rows = (
            (mixed[batch] - row_mean)
            * lax.rsqrt(spread + 1e-06)
            * (1.0 + modulation_ref[2:3, :])
            + modulation_ref[1:2, :]
        ).astype(jnp.bfloat16)
        normed_out[batch] = normed_rows
        for offset in range(1, chips):
            normed_copy(batch, offset).start()

        @pl.when(s != t)
        def _():
            normed_copy(batch, 0).start()

        @pl.when(s == t)
        def _():
            normed[batch, s] = normed_rows

    relays = []
    for batch in range(batches):
        for at in range(stages // 2):
            relay = relay_copy(batch, at, 2 * at + core)

            @pl.when(jnp.logical_or(t != s, s != 2 * at + core))
            def _():
                relay.wait_recv()

            relay.start()
            relays.append(relay)
    for batch in range(batches):
        for at in range(stages // 2):
            relay_copy(batch, at, 2 * at + 1 - core).wait_recv()
    for copy in up_copies:
        copy.wait()
    def active_copy(way, chunk):
        return remote(
            active.at[way, chunk],
            active.at[way, chunk],
            active_send.at[way, chunk],
            active_recv.at[way, chunk],
            t,
            s + (1 if way == 0 else -1),
        )

    def hidden_copy(way, chunk):
        return remote(
            hidden_out.at[way, chunk],
            hidden_in.at[way, chunk],
            hidden_send.at[way, chunk],
            hidden_recv.at[way, chunk],
            t,
            s + (-1 if way == 0 else 1),
        )

    def slot(at, carry):
        @pl.when(at < chunks)
        def _():
            product = jnp.dot(
                normed[...].reshape(2 * half, -1),
                up_weight[at],
                preferred_element_type=jnp.float32,
            )
            hidden_own[at] = product
            for way in range(2):

                @pl.when((s if way == 0 else stages - 1 - s) == stages - 1)
                def _():
                    block = product[way * half : (way + 1) * half, :]
                    hidden_out[way, at] = block.astype(jnp.bfloat16)
                    hidden_copy(way, at).start()

        for way in range(2):
            place = s if way == 0 else stages - 1 - s
            chunk = at - LAG * (stages - 1 - place)

            @pl.when(
                jnp.logical_and(
                    place < stages - 1, jnp.logical_and(chunk >= 0, chunk < chunks)
                )
            )
            def _():
                hidden_copy(way, chunk).wait_recv()
                combined = hidden_own[chunk, way * half : (way + 1) * half, :]
                combined = combined + hidden_in[way, chunk].astype(jnp.float32)

                @pl.when(place > 0)
                def _():
                    hidden_out[way, chunk] = combined.astype(jnp.bfloat16)
                    hidden_copy(way, chunk).start()

                @pl.when(place == 0)
                def _():
                    active[way, chunk] = jax.nn.gelu(combined, approximate=True).astype(
                        jnp.bfloat16
                    )
                    active_copy(way, chunk).start()

            back = at - LAG * (stages - 1 + place)

            @pl.when(jnp.logical_and(place > 0, jnp.logical_and(back >= 0, back < chunks)))
            def _():
                active_copy(way, back).wait_recv()

                @pl.when(place < stages - 1)
                def _():
                    active_copy(way, back).start()

            @pl.when(at == chunks - 1 + LAG * (stages - 1 + place))
            def _():
                finish(way)

        return carry

    def down_copy(way, offset):
        return remote(
            down_out.at[way, offset - 1],
            down_in.at[way, offset - 1],
            down_send.at[way, offset - 1],
            down_recv.at[way, offset - 1],
            lax.rem(t + offset, ranks),
            s,
        )

    def finish(way):
        total = None
        for chunk in range(chunks):
            product = contract_last(active[way, chunk], down_weight[chunk])
            total = product if total is None else total + product
        down_total[way] = total
        for offset in range(1, ranks):
            rank = lax.rem(t + offset, ranks)
            block = down_total[way, pl.ds(pl.multiple_of(rank * part, part), part), :]
            down_out[way, offset - 1] = block.astype(jnp.bfloat16)
            down_copy(way, offset).start()

    for copy in down_copies_in:
        copy.wait()
    lax.fori_loop(0, chunks + 2 * LAG * (stages - 1), slot, 0)


    def last_copy(way):
        return remote(
            last_out.at[way], last_in.at[way], last_send.at[way], last_recv.at[way], s, t
        )

    for way in range(2):
        summed = down_total[way, pl.ds(pl.multiple_of(t * part, part), part), :]
        for offset in range(1, ranks):
            down_copy(way, offset).wait_recv()
            summed = summed + down_in[way, offset - 1].astype(jnp.float32)
        last_out[way] = summed.astype(jnp.bfloat16)

        @pl.when(s != t)
        def _():
            last_copy(way).start()

        @pl.when(s == t)
        def _():
            last_in[way] = last_out[way]

    for way in range(2):

        @pl.when(s != t)
        def _():
            last_copy(way).wait_recv()

        result = mixed[way] + modulation_ref[3:4, :] * last_in[way].astype(jnp.float32)
        result_ref[way] = result.astype(jnp.bfloat16)

    for copy in head_copies[0] + head_copies[1] + attend_copies + project_copies + sums_copies:
        copy.wait_send()
    for relay in relays:
        relay.wait_send()
    for batch in range(batches):
        for offset in range(1, chips):
            normed_copy(batch, offset).wait_send()
        for offset in range(1, ranks):
            down_copy(batch, offset).wait_send()

        @pl.when(s != t)
        def _():
            normed_copy(batch, 0).wait_send()
            last_copy(batch).wait_send()

    def drain(chunk, carry):
        for way in range(2):
            place = s if way == 0 else stages - 1 - s

            @pl.when(place > 0)
            def _():
                hidden_copy(way, chunk).wait_send()

            @pl.when(place < stages - 1)
            def _():
                active_copy(way, chunk).wait_send()

        return carry

    lax.fori_loop(0, chunks, drain, 0)


def stationary(ranks, stages, *operands):
    query_rows, _, _, residual, _, out_weight, up_weight, down_weight = operands
    members = ranks * stages
    batches, few_tokens, inner = query_rows.shape
    width = inner // members
    tokens = few_tokens * members
    part = tokens // stages
    features = out_weight.shape[0]
    depth, hidden = up_weight.shape
    band = BAND
    chunks = hidden // band
    bands = (chunks, depth, band)
    half_type, dma = jnp.bfloat16, pltpu.SemaphoreType.DMA
    scratch = [
        *(pltpu.VMEM(operand.shape, operand.dtype) for operand in operands[:5]),
        pltpu.VMEM(out_weight.shape, half_type),
        pltpu.VMEM(bands, half_type),
        pltpu.VMEM(bands, half_type),
        pltpu.VMEM((3, batches, members, few_tokens, width), half_type),
        pltpu.VMEM((ranks, batches, tokens, width), half_type),
        pltpu.VMEM((batches, tokens, features), jnp.float32),
        pltpu.VMEM((batches, stages - 1, part, features), half_type),
        pltpu.VMEM((batches, stages - 1, part, features), half_type),
        pltpu.VMEM((batches, part, features), jnp.float32),
        pltpu.VMEM((batches, ranks, part, 128), jnp.float32),
        pltpu.VMEM((batches, part, features), half_type),
        pltpu.VMEM((batches, stages, part, depth), half_type),
        pltpu.VMEM((chunks, 2 * tokens, band), jnp.float32),
        pltpu.VMEM((2, chunks, tokens, band), half_type),
        pltpu.VMEM((2, chunks, tokens, band), half_type),
        pltpu.VMEM((2, chunks, tokens, band), half_type),
        pltpu.VMEM((batches, tokens, depth), jnp.float32),
        pltpu.VMEM((batches, ranks - 1, part, depth), half_type),
        pltpu.VMEM((batches, ranks - 1, part, depth), half_type),
        pltpu.VMEM((batches, part, depth), half_type),
        pltpu.VMEM((batches, part, depth), half_type),
        dma((5,)),
        dma,
        dma((2, chunks)),
        dma((batches, 3)),
        dma((batches, 3, members - 1)),
        dma((batches, 3, members - 1)),
        dma((batches, ranks - 1)),
        dma((batches, ranks)),
        dma((batches, stages - 1)),
        dma((batches, stages - 1)),
        dma((batches, ranks - 1)),
        dma((batches, ranks - 1)),
        dma((batches, ranks // 2)),
        dma((batches, stages)),
        dma((batches, stages // 2)),
        dma((2, chunks)),
        dma((2, chunks)),
        dma((2, chunks)),
        dma((2, chunks)),
        dma((batches, ranks - 1)),
        dma((batches, ranks - 1)),
        dma((batches,)),
        dma((batches,)),
    ]
    vmem = pl.BlockSpec(memory_space=pltpu.VMEM)
    return pl.pallas_call(
        functools.partial(block_kernel, ranks, stages, chunks),
        out_shape=jax.ShapeDtypeStruct(residual.shape, half_type),
        in_specs=[pl.BlockSpec(memory_space=pl.ANY)] * 8,
        out_specs=vmem,
        scratch_shapes=scratch,
        compiler_params=pltpu.CompilerParams(
            collective_id=0, has_side_effects=True, vmem_limit_bytes=62 * 1024 * 1024
        ),
    )(*operands)


def solution(mesh):
    in_specs = (
        P("groups", ("sp", "tp"), None),
        P("groups", ("sp", "tp"), None),
        P("groups", ("sp", "tp"), None),
        P("groups", "sp", "tp"),
        P(None, "tp"),
        P("tp", "sp"),
        P("sp", "tp"),
        P("sp", "tp"),
    )
    out_specs = P("groups", "sp", "tp")
    def block(*operands):
        sizes = mesh.shape
        rows = operands[0].shape[0] * operands[0].shape[1] * sizes["sp"] * sizes["tp"]
        square = sizes["sp"] == sizes["tp"] and sizes["sp"] % 2 == 0
        whole_heads = operands[0].shape[2] % (sizes["sp"] * sizes["tp"] * HEAD_FEATURES) == 0
        few = operands[6].shape[1] % BAND == 0 and rows < operands[6].shape[0]
        if square and whole_heads and few and operands[0].shape[0] == 2:
            return stationary(sizes["tp"], sizes["sp"], *operands)
        return body(*operands)

    return jax.shard_map(block, mesh=mesh, in_specs=in_specs, out_specs=out_specs, check_vma=False)
```

```python
import functools
import math

import jax
import jax.numpy as jnp
from jax import lax
from jax.experimental import pallas as pl
from jax.experimental.pallas import tpu as pltpu
from jax.sharding import PartitionSpec as P

D = 2560
HEAD_FEATURES = 128
BAND = 128
LAG = 5


def contract_last(left, right):
    return lax.dot_general(
        left, right, (((1,), (1,)), ((), ())), preferred_element_type=jnp.float32
    )


def attend(query_part, key_part, value_part):
    query_heads, key_heads, value_heads = (
        lax.all_to_all(query_part, "sp", split_axis=2, concat_axis=1, tiled=True),
        lax.all_to_all(key_part, "sp", split_axis=2, concat_axis=1, tiled=True),
        lax.all_to_all(value_part, "sp", split_axis=2, concat_axis=1, tiled=True),
    )
    batches, query_count, local_width = query_heads.shape
    local_heads = local_width // HEAD_FEATURES
    grouped = query_heads.reshape(batches, query_count, local_heads, HEAD_FEATURES)
    score_scale = 1.0 / math.sqrt(HEAD_FEATURES)

    def absorb_block(running, blocks):
        block_keys, block_values = blocks
        highest, row_total, weighted_values = running
        attention_logits = (
            jnp.einsum("bqhd,bkhd->bqhk", grouped, block_keys, preferred_element_type=jnp.float32)
            * score_scale
        )
        raised = jnp.maximum(highest, jnp.max(attention_logits, axis=-1))
        damping = jnp.exp(highest - raised)
        exponent = jnp.exp(attention_logits - raised[..., None])
        row_total = row_total * damping + jnp.sum(exponent, axis=-1)
        weighted_values = weighted_values * damping[..., None] + jnp.einsum(
            "bqhk,bkhd->bqhd",
            exponent.astype(jnp.bfloat16),
            block_values,
            preferred_element_type=jnp.float32,
        )
        return (raised, row_total, weighted_values)

    def scan_step(running, blocks):
        return (absorb_block(running, blocks), None)

    def absorb(running, section):
        key_section, value_section = section
        key_count = key_section.shape[1]
        shaped_keys = key_section.reshape(batches, key_count, local_heads, HEAD_FEATURES)
        shaped_values = value_section.reshape(batches, key_count, local_heads, HEAD_FEATURES)
        if key_count > 512 and key_count % 512 == 0:
            block_count = key_count // 512
            key_blocks = jnp.moveaxis(
                shaped_keys.reshape(batches, block_count, 512, local_heads, HEAD_FEATURES), 1, 0
            )
            value_blocks = jnp.moveaxis(
                shaped_values.reshape(batches, block_count, 512, local_heads, HEAD_FEATURES), 1, 0
            )
            running, unused = lax.scan(scan_step, running, (key_blocks, value_blocks))
            return running
        return absorb_block(running, (shaped_keys, shaped_values))

    starting = (
        jnp.full((batches, query_count, local_heads), -jnp.inf, jnp.float32),
        jnp.zeros((batches, query_count, local_heads), jnp.float32),
        jnp.zeros((batches, query_count, local_heads, HEAD_FEATURES), jnp.float32),
    )
    highest, row_total, weighted_values = absorb(
        starting,
        (
            lax.all_gather(key_heads, "tp", axis=1, tiled=True),
            lax.all_gather(value_heads, "tp", axis=1, tiled=True),
        ),
    )
    normalized = (weighted_values / row_total[..., None]).astype(jnp.bfloat16)
    ordered = normalized.reshape(batches, query_count, local_width)
    return lax.all_to_all(ordered, "sp", split_axis=1, concat_axis=2, tiled=True)


def body(
    query_rows, key_rows, value_rows, residual, modulation, out_weight, up_weight, down_weight
):
    attended = attend(query_rows, key_rows, value_rows)
    stripes = lax.all_gather(attended, "tp", axis=1, tiled=True)
    batches, rows_block, inner_width = stripes.shape
    row_count = batches * rows_block
    flat_rows = stripes.reshape(row_count, inner_width)
    local_width = out_weight.shape[0]
    columns = flat_rows
    projected = contract_last(columns, lax.all_gather(out_weight, "sp", axis=1, tiled=True))
    mixed_rows = (
        residual.reshape(row_count, local_width).astype(jnp.float32) + modulation[0] * projected
    )
    first_sum, second_sum = lax.psum(
        (jnp.sum(mixed_rows, axis=1), jnp.sum(mixed_rows * mixed_rows, axis=1)), "tp"
    )
    row_mean = first_sum / D
    spread = second_sum / D - row_mean * row_mean
    normed = (
        (mixed_rows - row_mean[:, None])
        * lax.rsqrt(spread[:, None] + 1e-06)
        * (1.0 + modulation[2])
        + modulation[1]
    ).astype(jnp.bfloat16)
    gathered = lax.all_gather(normed, "tp", axis=1, tiled=True)
    columns = gathered
    hidden = jnp.dot(
        columns,
        lax.all_gather(up_weight, "sp", axis=0, tiled=True),
        preferred_element_type=jnp.float32,
    )
    active = jax.nn.gelu(hidden, approximate=True).astype(jnp.bfloat16)
    partial_out = contract_last(active, lax.all_gather(down_weight, "sp", axis=0, tiled=True))
    summed = lax.psum_scatter(
        partial_out.astype(jnp.bfloat16), "tp", scatter_dimension=1, tiled=True
    ).astype(jnp.float32)
    result = (mixed_rows + modulation[3] * summed).astype(jnp.bfloat16)
    return result.reshape(batches, rows_block, local_width)


def block_kernel(
    ranks,
    stages,
    chunks,
    query_hbm,
    key_hbm,
    value_hbm,
    residual_hbm,
    modulation_hbm,
    out_hbm,
    up_hbm,
    down_hbm,
    result_ref,
    query_ref,
    key_ref,
    value_ref,
    residual_ref,
    modulation_ref,
    out_weight,
    up_weight,
    down_weight,
    heads,
    attended,
    projected,
    outgoing,
    incoming,
    mixed,
    sums,
    normed_out,
    normed,
    hidden_own,
    hidden_out,
    hidden_in,
    active,
    down_total,
    down_out,
    down_in,
    last_out,
    last_in,
    input_sem,
    out_sem,
    weight_sem,
    own_sem,
    head_send,
    head_recv,
    attend_send,
    attend_recv,
    project_send,
    project_recv,
    sums_send,
    sums_recv,
    normed_send,
    normed_recv,
    relay_send,
    hidden_send,
    hidden_recv,
    active_send,
    active_recv,
    down_send,
    down_recv,
    last_send,
    last_recv,
):
    t, s = lax.axis_index("tp"), lax.axis_index("sp")
    members = ranks * stages
    me = s * ranks + t
    core = lax.rem(t, 2)
    chip = lax.div(t, 2)
    chips = ranks // 2
    sibling = t + 1 - 2 * core
    batches, few_tokens, _ = query_ref.shape
    width = heads.shape[-1]
    tokens = members * few_tokens
    part = tokens // stages
    rows = batches * part
    half = tokens
    band = hidden_in.shape[-1]

    def remote(source, target, send, recv, rank, stage):
        return pltpu.make_async_remote_copy(
            src_ref=source,
            dst_ref=target,
            send_sem=send,
            recv_sem=recv,
            device_id={"tp": rank, "sp": stage},
            device_id_type=pl.DeviceIdType.MESH,
        )

    input_copies = [
        pltpu.make_async_copy(source, target, input_sem.at[at])
        for at, (source, target) in enumerate(
            (
                (query_hbm, query_ref),
                (key_hbm, key_ref),
                (value_hbm, value_ref),
                (residual_hbm, residual_ref),
                (modulation_hbm, modulation_ref),
            )
        )
    ]
    for copy in input_copies:
        copy.start()
    out_copy = pltpu.make_async_copy(out_hbm, out_weight, out_sem)
    up_copies, down_copies_in = (
        [
            pltpu.make_async_copy(
                source.at[:, chunk * band : (chunk + 1) * band],
                target.at[chunk],
                weight_sem.at[at, chunk],
            )
            for chunk in range(chunks)
        ]
        for at, (source, target) in enumerate(((up_hbm, up_weight), (down_hbm, down_weight)))
    )

    barrier = pltpu.get_barrier_semaphore()
    for offset in range(1, members):
        other = lax.rem(me + offset, members)
        pl.semaphore_signal(
            barrier,
            inc=1,
            device_id={"tp": lax.rem(other, ranks), "sp": lax.div(other, ranks)},
            device_id_type=pl.DeviceIdType.MESH,
        )
    for copy in input_copies:
        copy.wait()
    pl.semaphore_wait(barrier, members - 1)

    def head_copy(batch, at, source, offset):
        other = lax.rem(me + offset, members)
        columns = pl.ds(pl.multiple_of(other * width, width), width)
        return remote(
            source.at[batch, :, columns],
            heads.at[at, batch, me],
            head_send.at[batch, at, offset - 1],
            head_recv.at[batch, at, offset - 1],
            lax.rem(other, ranks),
            lax.div(other, ranks),
        )

    sources = (query_ref, key_ref, value_ref)
    head_copies = [
        [
            head_copy(batch, at, source, offset)
            for offset in range(1, members)
            for at, source in enumerate(sources)
        ]
        for batch in range(batches)
    ]
    own_columns = pl.ds(pl.multiple_of(me * width, width), width)
    own_copies = [
        pltpu.make_async_copy(
            source.at[batch, :, own_columns], heads.at[at, batch, me], own_sem.at[batch, at]
        )
        for batch in range(batches)
        for at, source in enumerate(sources)
    ]
    for copy in head_copies[0] + head_copies[1] + own_copies:
        copy.start()
    for copy in [out_copy, *up_copies, *down_copies_in]:
        copy.start()
    for copy in own_copies:
        copy.wait()

    def head_rows(at, batch, columns):
        loaded = heads[at, batch, :, :, columns].astype(jnp.float32)
        return loaded.reshape(tokens, HEAD_FEATURES).astype(jnp.bfloat16)

    score_scale = 1.0 / math.sqrt(HEAD_FEATURES)
    def attend_copy(batch, source, at, rank):
        return remote(
            attended.at[source, batch],
            attended.at[source, batch],
            attend_send.at[batch, at],
            attend_recv.at[batch, source],
            rank,
            s,
        )

    attend_copies = []
    for batch in range(batches):
        for copy in head_copies[batch]:
            copy.wait_recv()
        for head in range(width // HEAD_FEATURES):
            columns = slice(head * HEAD_FEATURES, (head + 1) * HEAD_FEATURES)
            scores = score_scale * contract_last(
                head_rows(0, batch, columns), head_rows(1, batch, columns)
            )
            exponent = jnp.exp(scores - jnp.max(scores, axis=-1, keepdims=True))
            row_total = jnp.sum(exponent, axis=-1, keepdims=True)
            weighted = jnp.dot(
                exponent.astype(jnp.bfloat16),
                head_rows(2, batch, columns),
                preferred_element_type=jnp.float32,
            )
            attended[t, batch, :, columns] = (weighted / row_total).astype(jnp.bfloat16)
        for offset in range(chips):
            rank = lax.rem(t + 2 * offset, ranks) if offset else sibling
            copy = attend_copy(batch, t, offset, rank)
            copy.start()
            attend_copies.append(copy)

    out_copy.wait()
    project_copies = []
    for batch in range(batches):
        for offset in range(1, chips):
            source = lax.rem(t + ranks - 2 * offset, ranks)
            copy = attend_copy(batch, source, chips - 1 + offset, sibling)
            copy.wait_recv()
            copy.start()
            attend_copies.append(copy)
        for offset in range(chips):
            source = lax.rem(sibling + ranks - 2 * offset, ranks)
            attend_copy(batch, source, 0, sibling).wait_recv()
        total = None
        for rank in range(ranks):
            columns = slice(rank * width, (rank + 1) * width)
            product = contract_last(attended[rank, batch], out_weight[:, columns])
            total = product if total is None else total + product
        projected[batch] = total
        for offset in range(1, stages):
            stage = lax.rem(s + offset, stages)
            block = projected[batch, pl.ds(pl.multiple_of(stage * part, part), part), :]
            outgoing[batch, offset - 1] = block.astype(jnp.bfloat16)
            copy = remote(
                outgoing.at[batch, offset - 1],
                incoming.at[batch, offset - 1],
                project_send.at[batch, offset - 1],
                project_recv.at[batch, offset - 1],
                t,
                stage,
            )
            copy.start()
            project_copies.append(copy)

    sums_copies = []
    lanes = lax.broadcasted_iota(jnp.int32, (part, 128), 1)
    for batch in range(batches):
        kept = projected[batch, pl.ds(pl.multiple_of(s * part, part), part), :]
        for offset in range(1, stages):
            project_copies[batch * (stages - 1) + offset - 1].wait_recv()
            kept = kept + incoming[batch, offset - 1].astype(jnp.float32)
        stream = residual_ref[batch].astype(jnp.float32) + modulation_ref[0:1, :] * kept
        mixed[batch] = stream
        first = jnp.sum(stream, axis=1, keepdims=True)
        second = jnp.sum(stream * stream, axis=1, keepdims=True)
        sums[batch, t] = jnp.where(lanes == 0, first, second)
        for offset in range(1, ranks):
            copy = remote(
                sums.at[batch, t],
                sums.at[batch, t],
                sums_send.at[batch, offset - 1],
                sums_recv.at[batch, offset - 1],
                lax.rem(t + offset, ranks),
                s,
            )
            copy.start()
            sums_copies.append(copy)

    own_core = lax.rem(s, 2)

    def normed_copy(batch, offset):
        return remote(
            normed_out.at[batch],
            normed.at[batch, s],
            normed_send.at[batch, offset],
            normed_recv.at[batch, s],
            2 * lax.rem(chip + offset, chips) + own_core,
            t,
        )

    def relay_copy(batch, at, source):
        block = normed.at[batch, source]
        return remote(
            block, block, relay_send.at[batch, at], normed_recv.at[batch, source], sibling, s
        )

    for batch in range(batches):
        for copy in sums_copies[batch * (ranks - 1) : (batch + 1) * (ranks - 1)]:
            copy.wait_recv()
        both_sums = sums[batch, 0]
        for rank in range(1, ranks):
            both_sums = both_sums + sums[batch, rank]
        row_mean = both_sums[:, 0:1] / D
        spread = both_sums[:, 1:2] / D - row_mean * row_mean
        normed_rows = (
            (mixed[batch] - row_mean)
            * lax.rsqrt(spread + 1e-06)
            * (1.0 + modulation_ref[2:3, :])
            + modulation_ref[1:2, :]
        ).astype(jnp.bfloat16)
        normed_out[batch] = normed_rows
        for offset in range(1, chips):
            normed_copy(batch, offset).start()

        @pl.when(s != t)
        def _():
            normed_copy(batch, 0).start()

        @pl.when(s == t)
        def _():
            normed[batch, s] = normed_rows

    relays = []
    for batch in range(batches):
        for at in range(stages // 2):
            relay = relay_copy(batch, at, 2 * at + core)

            @pl.when(jnp.logical_or(t != s, s != 2 * at + core))
            def _():
                relay.wait_recv()

            relay.start()
            relays.append(relay)
    for batch in range(batches):
        for at in range(stages // 2):
            relay_copy(batch, at, 2 * at + 1 - core).wait_recv()
    for copy in up_copies:
        copy.wait()
    def active_copy(way, chunk):
        return remote(
            active.at[way, chunk],
            active.at[way, chunk],
            active_send.at[way, chunk],
            active_recv.at[way, chunk],
            t,
            s + (1 if way == 0 else -1),
        )

    def hidden_copy(way, chunk):
        return remote(
            hidden_out.at[way, chunk],
            hidden_in.at[way, chunk],
            hidden_send.at[way, chunk],
            hidden_recv.at[way, chunk],
            t,
            s + (-1 if way == 0 else 1),
        )

    def slot(at, carry):
        @pl.when(at < chunks)
        def _():
            product = jnp.dot(
                normed[...].reshape(2 * half, -1),
                up_weight[at],
                preferred_element_type=jnp.float32,
            )
            hidden_own[at] = product
            for way in range(2):

                @pl.when((s if way == 0 else stages - 1 - s) == stages - 1)
                def _():
                    block = product[way * half : (way + 1) * half, :]
                    hidden_out[way, at] = block.astype(jnp.bfloat16)
                    hidden_copy(way, at).start()

        for way in range(2):
            place = s if way == 0 else stages - 1 - s
            chunk = at - LAG * (stages - 1 - place)

            @pl.when(
                jnp.logical_and(
                    place < stages - 1, jnp.logical_and(chunk >= 0, chunk < chunks)
                )
            )
            def _():
                hidden_copy(way, chunk).wait_recv()
                combined = hidden_own[chunk, way * half : (way + 1) * half, :]
                combined = combined + hidden_in[way, chunk].astype(jnp.float32)

                @pl.when(place > 0)
                def _():
                    hidden_out[way, chunk] = combined.astype(jnp.bfloat16)
                    hidden_copy(way, chunk).start()

                @pl.when(place == 0)
                def _():
                    active[way, chunk] = jax.nn.gelu(combined, approximate=True).astype(
                        jnp.bfloat16
                    )
                    active_copy(way, chunk).start()

            back = at - LAG * (stages - 1 + place)

            @pl.when(jnp.logical_and(place > 0, jnp.logical_and(back >= 0, back < chunks)))
            def _():
                active_copy(way, back).wait_recv()

                @pl.when(place < stages - 1)
                def _():
                    active_copy(way, back).start()

            @pl.when(at == early - 1 + LAG * (stages - 1 + place))
            def _():
                down_total[way] = down_product(way, 0, early)

            @pl.when(at == chunks - 1 + LAG * (stages - 1 + place))
            def _():
                finish(way)

        return carry

    def down_copy(way, offset):
        return remote(
            down_out.at[way, offset - 1],
            down_in.at[way, offset - 1],
            down_send.at[way, offset - 1],
            down_recv.at[way, offset - 1],
            lax.rem(t + offset, ranks),
            s,
        )

    early = chunks - chunks // 4

    def down_product(way, low, high):
        total = None
        for chunk in range(low, high):
            product = contract_last(active[way, chunk], down_weight[chunk])
            total = product if total is None else total + product
        return total

    def finish(way):
        down_total[way] += down_product(way, early, chunks)
        for offset in range(1, ranks):
            rank = lax.rem(t + offset, ranks)
            block = down_total[way, pl.ds(pl.multiple_of(rank * part, part), part), :]
            down_out[way, offset - 1] = block.astype(jnp.bfloat16)
            down_copy(way, offset).start()

    for copy in down_copies_in:
        copy.wait()
    lax.fori_loop(0, chunks + 2 * LAG * (stages - 1), slot, 0)


    def last_copy(way):
        return remote(
            last_out.at[way], last_in.at[way], last_send.at[way], last_recv.at[way], s, t
        )

    for way in range(2):
        summed = down_total[way, pl.ds(pl.multiple_of(t * part, part), part), :]
        for offset in range(1, ranks):
            down_copy(way, offset).wait_recv()
            summed = summed + down_in[way, offset - 1].astype(jnp.float32)
        last_out[way] = summed.astype(jnp.bfloat16)

        @pl.when(s != t)
        def _():
            last_copy(way).start()

        @pl.when(s == t)
        def _():
            last_in[way] = last_out[way]

    for way in range(2):

        @pl.when(s != t)
        def _():
            last_copy(way).wait_recv()

        result = mixed[way] + modulation_ref[3:4, :] * last_in[way].astype(jnp.float32)
        result_ref[way] = result.astype(jnp.bfloat16)

    for copy in head_copies[0] + head_copies[1] + attend_copies + project_copies + sums_copies:
        copy.wait_send()
    for relay in relays:
        relay.wait_send()
    for batch in range(batches):
        for offset in range(1, chips):
            normed_copy(batch, offset).wait_send()
        for offset in range(1, ranks):
            down_copy(batch, offset).wait_send()

        @pl.when(s != t)
        def _():
            normed_copy(batch, 0).wait_send()
            last_copy(batch).wait_send()

    def drain(chunk, carry):
        for way in range(2):
            place = s if way == 0 else stages - 1 - s

            @pl.when(place > 0)
            def _():
                hidden_copy(way, chunk).wait_send()

            @pl.when(place < stages - 1)
            def _():
                active_copy(way, chunk).wait_send()

        return carry

    lax.fori_loop(0, chunks, drain, 0)


def stationary(ranks, stages, *operands):
    query_rows, _, _, residual, _, out_weight, up_weight, down_weight = operands
    members = ranks * stages
    batches, few_tokens, inner = query_rows.shape
    width = inner // members
    tokens = few_tokens * members
    part = tokens // stages
    features = out_weight.shape[0]
    depth, hidden = up_weight.shape
    band = BAND
    chunks = hidden // band
    bands = (chunks, depth, band)
    half_type, dma = jnp.bfloat16, pltpu.SemaphoreType.DMA
    scratch = [
        *(pltpu.VMEM(operand.shape, operand.dtype) for operand in operands[:5]),
        pltpu.VMEM(out_weight.shape, half_type),
        pltpu.VMEM(bands, half_type),
        pltpu.VMEM(bands, half_type),
        pltpu.VMEM((3, batches, members, few_tokens, width), half_type),
        pltpu.VMEM((ranks, batches, tokens, width), half_type),
        pltpu.VMEM((batches, tokens, features), jnp.float32),
        pltpu.VMEM((batches, stages - 1, part, features), half_type),
        pltpu.VMEM((batches, stages - 1, part, features), half_type),
        pltpu.VMEM((batches, part, features), jnp.float32),
        pltpu.VMEM((batches, ranks, part, 128), jnp.float32),
        pltpu.VMEM((batches, part, features), half_type),
        pltpu.VMEM((batches, stages, part, depth), half_type),
        pltpu.VMEM((chunks, 2 * tokens, band), jnp.float32),
        pltpu.VMEM((2, chunks, tokens, band), half_type),
        pltpu.VMEM((2, chunks, tokens, band), half_type),
        pltpu.VMEM((2, chunks, tokens, band), half_type),
        pltpu.VMEM((batches, tokens, depth), jnp.float32),
        pltpu.VMEM((batches, ranks - 1, part, depth), half_type),
        pltpu.VMEM((batches, ranks - 1, part, depth), half_type),
        pltpu.VMEM((batches, part, depth), half_type),
        pltpu.VMEM((batches, part, depth), half_type),
        dma((5,)),
        dma,
        dma((2, chunks)),
        dma((batches, 3)),
        dma((batches, 3, members - 1)),
        dma((batches, 3, members - 1)),
        dma((batches, ranks - 1)),
        dma((batches, ranks)),
        dma((batches, stages - 1)),
        dma((batches, stages - 1)),
        dma((batches, ranks - 1)),
        dma((batches, ranks - 1)),
        dma((batches, ranks // 2)),
        dma((batches, stages)),
        dma((batches, stages // 2)),
        dma((2, chunks)),
        dma((2, chunks)),
        dma((2, chunks)),
        dma((2, chunks)),
        dma((batches, ranks - 1)),
        dma((batches, ranks - 1)),
        dma((batches,)),
        dma((batches,)),
    ]
    vmem = pl.BlockSpec(memory_space=pltpu.VMEM)
    return pl.pallas_call(
        functools.partial(block_kernel, ranks, stages, chunks),
        out_shape=jax.ShapeDtypeStruct(residual.shape, half_type),
        in_specs=[pl.BlockSpec(memory_space=pl.ANY)] * 8,
        out_specs=vmem,
        scratch_shapes=scratch,
        compiler_params=pltpu.CompilerParams(
            collective_id=0, has_side_effects=True, vmem_limit_bytes=62 * 1024 * 1024
        ),
    )(*operands)


def solution(mesh):
    in_specs = (
        P("groups", ("sp", "tp"), None),
        P("groups", ("sp", "tp"), None),
        P("groups", ("sp", "tp"), None),
        P("groups", "sp", "tp"),
        P(None, "tp"),
        P("tp", "sp"),
        P("sp", "tp"),
        P("sp", "tp"),
    )
    out_specs = P("groups", "sp", "tp")
    def block(*operands):
        sizes = mesh.shape
        rows = operands[0].shape[0] * operands[0].shape[1] * sizes["sp"] * sizes["tp"]
        square = sizes["sp"] == sizes["tp"] and sizes["sp"] % 2 == 0
        whole_heads = operands[0].shape[2] % (sizes["sp"] * sizes["tp"] * HEAD_FEATURES) == 0
        few = operands[6].shape[1] >= 4 * BAND and operands[6].shape[1] % BAND == 0 and rows < operands[6].shape[0]
        if square and whole_heads and few and operands[0].shape[0] == 2:
            return stationary(sizes["tp"], sizes["sp"], *operands)
        return body(*operands)

    return jax.shard_map(block, mesh=mesh, in_specs=in_specs, out_specs=out_specs, check_vma=False)
```
